32 devices in a mesh: part: 1 (over z), tp: 4 (over y), dp: 8 (over x, core).
Axes of the slice: x: 4, y: 4, z: 1, core: 2. Of those that a mesh axis runs over, the one named last changes fastest.
The devices are a block of a 4x4x8 slice.
Arguments:
- hidden: bfloat16 [128, 512, 768], P(('part', 'dp', 'tp'))
- ln_gain: float32 [768], replicated
- w_in: bfloat16 [768, 7040], P(None, ('dp', 'tp'))
- w_out: bfloat16 [3840, 768], P(('dp', 'tp'))
Outputs:
- output 1: bfloat16 [128, 512, 768], P(('part', 'dp', 'tp'))
- output 2: bfloat16 [128, 512, 64], P(('part', 'dp', 'tp'))
- output 3: bfloat16 [128, 512, 64], P(('part', 'dp', 'tp'))
All inputs are finite; a program needn't handle non-finite values.
Results may differ from the reference program's by a relative error of at most 0.00375414.
Values are sent between devices in bfloat16 or wider.
A program may use at most 768 MiB of HBM per device.

```python
import jax
import jax.numpy as jnp
from jax import lax

D = 768
HEADS = 12
HEAD = 64
BATCH = 128
SEQ = 512

FF = 4 * D
Q_WIDTH = HEADS * HEAD
JOINT = Q_WIDTH + 2 * HEAD + 2 * FF
MIXED = Q_WIDTH + FF
Q_BLOCK = min(SEQ, 512)
LN_EPS = 1e-6
ROPE_BASE = 10000.0
ATTN_GAIN = 3.0


def setup_inputs(seed: int = 0, part: int = 0) -> dict:
    root_key = jax.random.key(seed)
    key_hidden, key_gain, key_in, key_out = jax.random.split(root_key, 4)
    key_hidden = jax.random.fold_in(key_hidden, part)
    hidden = jax.random.normal(key_hidden, (BATCH, SEQ, D), jnp.float32)
    ln_gain = 1.0 + 0.25 * jax.random.normal(key_gain, (D,), jnp.float32)
    w_in = jax.random.normal(key_in, (D, JOINT), jnp.float32) * D ** -0.5
    row_scale = jnp.where(jnp.arange(MIXED) < Q_WIDTH, ATTN_GAIN, 1.0) * MIXED ** -0.5
    w_out = jax.random.normal(key_out, (MIXED, D), jnp.float32) * row_scale[:, None]
    return {'hidden': hidden.astype(jnp.bfloat16), 'ln_gain': ln_gain,
            'w_in': w_in.astype(jnp.bfloat16), 'w_out': w_out.astype(jnp.bfloat16)}


def rotate(values):
    half_dim = HEAD // 2
    inv_freq = ROPE_BASE ** (-jnp.arange(half_dim, dtype=jnp.float32) * 2.0 / HEAD)
    angles = jnp.arange(SEQ, dtype=jnp.float32)[:, None] * inv_freq[None, :]
    tab_shape = (SEQ,) + (1,) * (values.ndim - 2) + (half_dim,)
    cos_tab = jnp.cos(angles).reshape(tab_shape)
    sin_tab = jnp.sin(angles).reshape(tab_shape)
    first_half = values[..., :half_dim]
    second_half = values[..., half_dim:]
    return jnp.concatenate([first_half * cos_tab - second_half * sin_tab,
                            second_half * cos_tab + first_half * sin_tab], axis=-1)


def attention(q_rot, k_rot, v_seq):
    k_wide = k_rot.astype(jnp.float32)
    v_wide = v_seq.astype(jnp.float32)
    key_pos = jnp.arange(SEQ)
    q_blocks = q_rot.reshape(SEQ // Q_BLOCK, Q_BLOCK, HEADS, HEAD)

    def one_block(item):
        blk_idx, q_tile = item
        scores = jnp.einsum('qhe,ke->qhk', q_tile.astype(jnp.float32), k_wide) * HEAD ** -0.5
        q_pos = blk_idx * Q_BLOCK + jnp.arange(Q_BLOCK)
        allowed = key_pos[None, :] <= q_pos[:, None]
        scores = jnp.where(allowed[:, None, :], scores, -1e30)
        attn_prob = jax.nn.softmax(scores, axis=-1).astype(jnp.bfloat16)
        return jnp.einsum('qhk,ke->qhe', attn_prob.astype(jnp.float32), v_wide).astype(jnp.bfloat16)

    out_tiles = lax.map(one_block, (jnp.arange(SEQ // Q_BLOCK), q_blocks))
    return out_tiles.reshape(SEQ, Q_WIDTH)


def reference(hidden, ln_gain, w_in, w_out):
    def one_request(x_seq):
        x_wide = x_seq.astype(jnp.float32)
        centered = x_wide - jnp.mean(x_wide, axis=-1, keepdims=True)
        row_var = jnp.mean(centered * centered, axis=-1, keepdims=True)
        h_seq = (centered * lax.rsqrt(row_var + LN_EPS) * ln_gain).astype(jnp.bfloat16)
        joint_out = jnp.dot(h_seq, w_in, preferred_element_type=jnp.float32).astype(jnp.bfloat16)
        q_raw = joint_out[:, :Q_WIDTH].reshape(SEQ, HEADS, HEAD)
        k_raw = joint_out[:, Q_WIDTH:Q_WIDTH + HEAD]
        v_seq = joint_out[:, Q_WIDTH + HEAD:Q_WIDTH + 2 * HEAD]
        gate_proj = joint_out[:, Q_WIDTH + 2 * HEAD:Q_WIDTH + 2 * HEAD + FF]
        up_proj = joint_out[:, Q_WIDTH + 2 * HEAD + FF:]
        q_rot = rotate(q_raw.astype(jnp.float32)).astype(jnp.bfloat16)
        k_rot = rotate(k_raw.astype(jnp.float32)).astype(jnp.bfloat16)
        attn_out = attention(q_rot, k_rot, v_seq)
        mlp_out = (jax.nn.silu(gate_proj.astype(jnp.float32)) * up_proj.astype(jnp.float32)).astype(jnp.bfloat16)
        mixed_rows = jnp.concatenate([attn_out, mlp_out], axis=-1)
        proj_out = jnp.dot(mixed_rows, w_out, preferred_element_type=jnp.float32)
        y_seq = (x_wide + proj_out).astype(jnp.bfloat16)
        return (y_seq, k_rot, v_seq)

    y_all, k_all, v_all = lax.map(one_request, hidden)
    return (y_all, k_all, v_all)
```

```python
import functools

import jax
import jax.numpy as jnp
import numpy as np
from jax import lax
from jax.experimental import pallas as pl
from jax.experimental.pallas import tpu as pltpu
from jax.sharding import PartitionSpec as P

LN_EPS = 1e-6
ROPE_BASE = 10000.0
MESH = pl.DeviceIdType.MESH
F32 = jnp.float32
BF16 = jnp.bfloat16


def nt_dot(lhs, rhs):
    return lax.dot_general(lhs, rhs, (((1,), (1,)), ((), ())), preferred_element_type=F32)


class Ring:
    def __init__(self, n, pos, right, left, block, send, recv):
        self.n, self.pos, self.right, self.left = n, pos, right, left
        self.block, self.send, self.recv = block, send, recv
        self.routes = ((0, 0, True), (0, 1, True), (1, 0, True), (0, 1, False), (0, 0, False), (1, 1, False))

    def _copy(self, k, hops):
        back, half, to_right = self.routes[k]
        step = (back + hops) if to_right else self.n - (back + hops)
        z = lax.rem(self.pos - step + 2 * self.n, self.n)
        ref = self.block(z, half)
        return pltpu.make_async_remote_copy(
            src_ref=ref, dst_ref=ref, send_sem=self.send(k), recv_sem=self.recv(k),
            device_id=self.right if to_right else self.left, device_id_type=MESH)

    def start(self):
        for k in (0, 3, 1, 4):
            self._copy(k, 0).start()

    def forward(self):
        self._copy(0, 1).wait_recv()
        self._copy(2, 0).start()
        self._copy(3, 1).wait_recv()
        self._copy(5, 0).start()

    def finish(self):
        for k in (1, 4, 2, 5):
            self._copy(k, 1).wait_recv()

    def drain(self):
        for k in range(6):
            self._copy(k, 0).wait_send()


def layer_kernel(n, x_hbm, gain_ref, wi_hbm, wo_hbm, cos_ref, sin_ref, y_hbm, kc_ref, vc_ref,
                 x_v, h_v, mixed, gi, go, wq, wg, wu, wo, qkv, kt,
                 x_sem, own_sem, y_sem, send_sem, recv_sem, psend_sem, precv_sem):
    n_req, seq, d = x_v.shape
    in_rows, half = gi.shape[2], gi.shape[3]
    out_rows = go.shape[2]
    n_dev = gi.shape[1]
    head = kc_ref.shape[1]
    q_width = wq.shape[0] - 2 * head
    ff = wo.shape[0] - q_width
    chunk = wg.shape[0]

    dp, tp = lax.axis_index("dp"), lax.axis_index("tp")
    core, x, y = lax.rem(dp, 2), dp // 2, tp
    a = (1 - core) * x + core * y
    b = (1 - core) * y + core * x

    def place(za, zb, c):
        zx = (1 - c) * za + c * zb
        zy = (1 - c) * zb + c * za
        return zx * 2 + c, zy

    def device(za, zb):
        zdp, ztp = place(lax.rem(za + n, n), lax.rem(zb + n, n), core)
        return {"dp": zdp, "tp": ztp}

    def shard(za, zb, c):
        zdp, ztp = place(za, zb, c)
        return zdp * n + ztp

    partner = {"dp": x * 2 + 1 - core, "tp": tp}
    bufs = (gi, go)
    me = dp * n + tp

    own = []
    for h in range(2):
        own.append(pltpu.make_async_copy(wi_hbm.at[:, pl.ds(h * half, half)], gi.at[h, me], own_sem.at[0, h]))
    for h in range(2):
        own.append(pltpu.make_async_copy(wo_hbm.at[:, pl.ds(h * half, half)], go.at[h, me], own_sem.at[1, h]))
    for copy in own:
        copy.start()
    x_in = [pltpu.make_async_copy(x_hbm.at[r], x_v.at[r], x_sem.at[r]) for r in range(n_req)]
    for copy in x_in:
        copy.start()

    barrier = pltpu.get_barrier_semaphore()
    for dev in (device(a + 1, b), device(a - 1, b), device(a, b + 1), device(a, b - 1), partner):
        pl.semaphore_signal(barrier, inc=1, device_id=dev, device_id_type=MESH)
    pl.semaphore_wait(barrier, 5)
    for copy in own:
        copy.wait()

    def first_ring(rnd):
        return Ring(n, a, device(a + 1, b), device(a - 1, b),
                    lambda z, h: bufs[rnd].at[h, shard(z, b, core)],
                    lambda k: send_sem.at[rnd, 0, k], lambda k: recv_sem.at[rnd, 0, k])

    def second_ring(rnd, s):
        return Ring(n, b, device(a, b + 1), device(a, b - 1),
                    lambda z, h: bufs[rnd].at[h, shard(s, z, core)],
                    lambda k: send_sem.at[rnd, 1 + s, k], lambda k: recv_sem.at[rnd, 1 + s, k])

    def pair_copy(rnd, s, k, mine):
        if mine:
            idx = shard(s, lax.rem(b + k, n), core)
        else:
            idx = shard(s, lax.rem(a + k, n), 1 - core)
        ref = bufs[rnd].at[:, idx]
        return pltpu.make_async_remote_copy(
            src_ref=ref, dst_ref=ref, send_sem=psend_sem.at[rnd, s, k], recv_sem=precv_sem.at[rnd, s, k],
            device_id=partner, device_id_type=MESH)

    firsts = [first_ring(r) for r in range(2)]
    seconds = [[second_ring(r, s) for s in range(n)] for r in range(2)]

    def finish_second(rnd, s):
        seconds[rnd][s].finish()
        for k in range(1, n):
            pair_copy(rnd, s, k, True).start()

    def start_second(rnd, s):
        seconds[rnd][s].start()
        pair_copy(rnd, s, 0, True).start()

    def from_partner(rnd, s):
        for k in range(n):
            pair_copy(rnd, s, k, False).wait_recv()

    firsts[0].start()

    gain = gain_ref[...]
    ln_rows = 128

    def norm_rows(r):
        def body(i, carry):
            rows = pl.ds(pl.multiple_of(i * ln_rows, ln_rows), ln_rows)
            xw = x_v[r, rows, :].astype(F32)
            cen = xw - jnp.mean(xw, axis=-1, keepdims=True)
            var = jnp.mean(cen * cen, axis=-1, keepdims=True)
            h_v[r, rows, :] = (cen * lax.rsqrt(var + LN_EPS) * gain).astype(BF16)
            return carry
        lax.fori_loop(0, seq // ln_rows, body, 0)

    x_in[0].wait()
    norm_rows(0)
    firsts[0].forward()
    x_in[1].wait()
    norm_rows(1)
    firsts[0].finish()
    start_second(0, 0)
    for r in range(2, n_req):
        x_in[r].wait()
        norm_rows(r)
    seconds[0][0].forward()
    for s in range(1, n):
        start_second(0, s)
    finish_second(0, 0)
    from_partner(0, 0)

    def assemble(dst, src, rows_per, start, count):
        row = start
        while row < start + count:
            blk, r0 = row // rows_per, row % rows_per
            take = min(rows_per - r0, start + count - row)
            for h in range(2):
                dst[row - start:row - start + take, h * half:(h + 1) * half] = src[h, blk, r0:r0 + take, :]
            row += take

    assemble(wq, gi, in_rows, 0, q_width + 2 * head)

    hd2 = head // 2
    scale = head ** -0.5
    qb = seq // 2
    key_idx = lax.broadcasted_iota(jnp.int32, (qb, qb), 0)
    qry_idx = lax.broadcasted_iota(jnp.int32, (qb, qb), 1)

    def rotate(u):
        cos, sin = cos_ref[...], sin_ref[...]
        first, second = u[:hd2].astype(F32), u[hd2:].astype(F32)
        return jnp.concatenate([first * cos - second * sin, second * cos + first * sin], axis=0).astype(BF16)

    def softmax_pv(blocks, vt):
        top = functools.reduce(jnp.maximum, [jnp.max(s, axis=0, keepdims=True) for s in blocks])
        probs = [jnp.exp((s - top) * scale) for s in blocks]
        total = functools.reduce(jnp.add, [jnp.sum(p, axis=0, keepdims=True) for p in probs])
        wide = probs[0] if len(probs) == 1 else jnp.concatenate(probs, axis=0)
        out = jnp.dot(vt, wide.astype(BF16), preferred_element_type=F32)
        return out / total

    def attend(r):
        h_r = h_v[r]
        qkv[...] = nt_dot(wq[...], h_r).astype(BF16)
        k_rot = rotate(qkv[q_width:q_width + head, :])
        kc_ref[r] = k_rot
        vc_ref[r] = qkv[q_width + head:, :]
        kt[...] = k_rot.astype(F32).T.astype(BF16)

        def one_head(row):
            q_rot = rotate(qkv[pl.ds(row, head), :])
            vt = vc_ref[r]
            s_a = jnp.dot(kt[:qb], q_rot[:, :qb], preferred_element_type=F32)
            s_b = jnp.dot(kt[:qb], q_rot[:, qb:], preferred_element_type=F32)
            s_c = jnp.dot(kt[qb:], q_rot[:, qb:], preferred_element_type=F32)
            allowed = key_idx <= qry_idx
            o_a = softmax_pv([jnp.where(allowed, s_a, -1e30)], vt[:, :qb])
            o_b = softmax_pv([s_b, jnp.where(allowed, s_c, -1e30)], vt)
            return jnp.concatenate([o_a, o_b], axis=1)

        def body(i, carry):
            row = pl.multiple_of(i * 2 * head, 2 * head)
            pair = jnp.concatenate([one_head(row), one_head(row + head)], axis=0)
            mixed[r, :, pl.ds(row, 2 * head)] = pair.T.astype(BF16)
            return carry

        lax.fori_loop(0, q_width // (2 * head), body, 0)

    attend(0)
    seconds[0][1].forward()
    firsts[1].start()
    attend(1)
    finish_second(0, 1)
    seconds[0][2].forward()
    seconds[0][3].forward()
    attend(2)
    finish_second(0, 2)
    finish_second(0, 3)
    firsts[1].forward()
    attend(3)
    firsts[1].finish()
    for s in range(n):
        start_second(1, s)
    for s in range(1, n):
        from_partner(0, s)

    gate_at = q_width + 2 * head
    tok = 256
    tiles = seq // tok

    def mlp_chunk(c):
        assemble(wg, gi, in_rows, gate_at + c * chunk, chunk)
        assemble(wu, gi, in_rows, gate_at + ff + c * chunk, chunk)

        def body(i, carry):
            r = i // tiles
            rows = pl.ds(pl.multiple_of((i - r * tiles) * tok, tok), tok)
            h_t = h_v[r, rows, :]
            g = nt_dot(h_t, wg[...]).astype(BF16).astype(F32)
            u = nt_dot(h_t, wu[...]).astype(BF16).astype(F32)
            act = 0.5 * g * (1.0 + jnp.tanh(0.5 * g))
            mixed[r, rows, q_width + c * chunk:q_width + (c + 1) * chunk] = (act * u).astype(BF16)
            return carry
        lax.fori_loop(0, n_req * tiles, body, 0)

    for c in range(ff // chunk):
        mlp_chunk(c)
        if c < n:
            seconds[1][c].forward()
        if 1 <= c <= n:
            finish_second(1, c - 1)
    for s in range(n):
        from_partner(1, s)

    assemble(wo, go, out_rows, 0, q_width + ff)

    def y_copy(r, t):
        rows = pl.ds(pl.multiple_of(t * tok, tok), tok)
        return pltpu.make_async_copy(x_v.at[r, rows], y_hbm.at[r, rows], y_sem.at[r, t])

    def out_body(i, carry):
        r = i // tiles
        t = i - r * tiles
        rows = pl.ds(pl.multiple_of(t * tok, tok), tok)
        acc = jnp.dot(mixed[r, rows, :], wo[...], preferred_element_type=F32)
        x_v[r, rows, :] = (x_v[r, rows, :].astype(F32) + acc).astype(BF16)
        y_copy(r, t).start()
        return carry
    lax.fori_loop(0, n_req * tiles, out_body, 0)

    for r in range(n_req):
        for t in range(tiles):
            y_copy(r, t).wait()
    for rnd in range(2):
        firsts[rnd].drain()
        for s in range(n):
            seconds[rnd][s].drain()
            for k in range(n):
                pair_copy(rnd, s, k, True).wait_send()


def rope_tables(seq, head):
    inv_freq = (np.float32(ROPE_BASE) ** (-np.arange(head // 2, dtype=np.float32) * np.float32(2.0) / np.float32(head)))
    angles = inv_freq.astype(np.float32)[:, None] * np.arange(seq, dtype=np.float32)[None, :]
    return np.cos(angles).astype(np.float32), np.sin(angles).astype(np.float32)


def solution(mesh):
    tok_spec = P(('part', 'dp', 'tp'))
    n = mesh.shape['tp']
    n_dev = n * mesh.shape['dp']

    def per_device(x_blk, ln_gain, w_in_blk, w_out_blk):
        n_req, seq, d = x_blk.shape
        in_rows, out_rows = w_in_blk.shape[1], w_out_blk.shape[0]
        ff = 4 * d
        q_width = out_rows * n_dev - ff
        head = (in_rows * n_dev - q_width - 2 * ff) // 2
        chunk = min(512, ff)
        cos, sin = rope_tables(seq, head)
        vmem = pl.BlockSpec(memory_space=pltpu.VMEM)
        anyw = pl.BlockSpec(memory_space=pl.ANY)
        tiles = seq // 256
        y, kc, vc = pl.pallas_call(
            functools.partial(layer_kernel, n),
            out_shape=(jax.ShapeDtypeStruct(x_blk.shape, BF16),
                       jax.ShapeDtypeStruct((n_req, head, seq), BF16),
                       jax.ShapeDtypeStruct((n_req, head, seq), BF16)),
            in_specs=[anyw, vmem, anyw, anyw, vmem, vmem],
            out_specs=(anyw, vmem, vmem),
            scratch_shapes=[
                pltpu.VMEM((n_req, seq, d), BF16),
                pltpu.VMEM((n_req, seq, d), BF16),
                pltpu.VMEM((n_req, seq, q_width + ff), BF16),
                pltpu.VMEM((2, n_dev, in_rows, d // 2), BF16),
                pltpu.VMEM((2, n_dev, out_rows, d // 2), BF16),
                pltpu.VMEM((q_width + 2 * head, d), BF16),
                pltpu.VMEM((chunk, d), BF16),
                pltpu.VMEM((chunk, d), BF16),
                pltpu.VMEM((q_width + ff, d), BF16),
                pltpu.VMEM((q_width + 2 * head, seq), BF16),
                pltpu.VMEM((seq, head), BF16),
                pltpu.SemaphoreType.DMA((n_req,)),
                pltpu.SemaphoreType.DMA((2, 2)),
                pltpu.SemaphoreType.DMA((n_req, tiles)),
                pltpu.SemaphoreType.DMA((2, 1 + n, 6)),
                pltpu.SemaphoreType.DMA((2, 1 + n, 6)),
                pltpu.SemaphoreType.DMA((2, n, n)),
                pltpu.SemaphoreType.DMA((2, n, n)),
            ],
            compiler_params=pltpu.CompilerParams(
                collective_id=0, has_side_effects=True, vmem_limit_bytes=63 * 1024 * 1024),
        )(x_blk, ln_gain.reshape(1, d), w_in_blk.T, w_out_blk, cos, sin)
        return y, kc.swapaxes(1, 2), vc.swapaxes(1, 2)

    return jax.shard_map(per_device, mesh=mesh,
                         in_specs=(tok_spec, P(), P(None, ('dp', 'tp')), P(('dp', 'tp'), None)),
                         out_specs=(tok_spec, tok_spec, tok_spec), check_vma=False)
```

```python
import functools

import jax
import jax.numpy as jnp
import numpy as np
from jax import lax
from jax.experimental import pallas as pl
from jax.experimental.pallas import tpu as pltpu
from jax.sharding import PartitionSpec as P

LN_EPS = 1e-6
ROPE_BASE = 10000.0
MESH = pl.DeviceIdType.MESH
F32 = jnp.float32
BF16 = jnp.bfloat16


def nt_dot(lhs, rhs):
    return lax.dot_general(lhs, rhs, (((1,), (1,)), ((), ())), preferred_element_type=F32)


class Ring:
    def __init__(self, n, pos, right, left, block, send, recv):
        self.n, self.pos, self.right, self.left = n, pos, right, left
        self.block, self.send, self.recv = block, send, recv
        self.routes = ((0, 0, True), (0, 1, True), (1, 0, True), (0, 1, False), (0, 0, False), (1, 1, False))

    def _copy(self, k, hops):
        back, half, to_right = self.routes[k]
        step = (back + hops) if to_right else self.n - (back + hops)
        z = lax.rem(self.pos - step + 2 * self.n, self.n)
        ref = self.block(z, half)
        return pltpu.make_async_remote_copy(
            src_ref=ref, dst_ref=ref, send_sem=self.send(k), recv_sem=self.recv(k),
            device_id=self.right if to_right else self.left, device_id_type=MESH)

    def start(self):
        for k in (0, 3, 1, 4):
            self._copy(k, 0).start()

    def forward(self):
        self._copy(0, 1).wait_recv()
        self._copy(2, 0).start()
        self._copy(3, 1).wait_recv()
        self._copy(5, 0).start()

    def finish(self):
        for k in (1, 4, 2, 5):
            self._copy(k, 1).wait_recv()

    def drain(self):
        for k in range(6):
            self._copy(k, 0).wait_send()


def layer_kernel(n, x_hbm, gain_ref, wi_hbm, wo_hbm, cos_ref, sin_ref, y_hbm, kc_ref, vc_ref,
                 x_v, h_v, mixed, gi, go, wq, wg, wu, wo, qkv, kt, s_a, s_b,
                 x_sem, own_sem, y_sem, send_sem, recv_sem, psend_sem, precv_sem):
    n_req, seq, d = x_v.shape
    in_rows, half = gi.shape[2], gi.shape[3]
    out_rows = go.shape[2]
    n_dev = gi.shape[1]
    head = kc_ref.shape[1]
    q_width = wq.shape[0] - 2 * head
    ff = wo.shape[0] - q_width
    chunk = wg.shape[0]

    dp, tp = lax.axis_index("dp"), lax.axis_index("tp")
    core, x, y = lax.rem(dp, 2), dp // 2, tp
    a = (1 - core) * x + core * y
    b = (1 - core) * y + core * x

    def place(za, zb, c):
        zx = (1 - c) * za + c * zb
        zy = (1 - c) * zb + c * za
        return zx * 2 + c, zy

    def device(za, zb):
        zdp, ztp = place(lax.rem(za + n, n), lax.rem(zb + n, n), core)
        return {"dp": zdp, "tp": ztp}

    def shard(za, zb, c):
        zdp, ztp = place(za, zb, c)
        return zdp * n + ztp

    partner = {"dp": x * 2 + 1 - core, "tp": tp}
    bufs = (gi, go)
    me = dp * n + tp

    own = []
    for h in range(2):
        own.append(pltpu.make_async_copy(wi_hbm.at[:, pl.ds(h * half, half)], gi.at[h, me], own_sem.at[0, h]))
    for h in range(2):
        own.append(pltpu.make_async_copy(wo_hbm.at[:, pl.ds(h * half, half)], go.at[h, me], own_sem.at[1, h]))
    for copy in own:
        copy.start()
    x_in = [pltpu.make_async_copy(x_hbm.at[r], x_v.at[r], x_sem.at[r]) for r in range(n_req)]
    for copy in x_in:
        copy.start()

    barrier = pltpu.get_barrier_semaphore()
    for dev in (device(a + 1, b), device(a - 1, b), device(a, b + 1), device(a, b - 1), partner):
        pl.semaphore_signal(barrier, inc=1, device_id=dev, device_id_type=MESH)
    pl.semaphore_wait(barrier, 5)
    for copy in own:
        copy.wait()

    def first_ring(rnd):
        return Ring(n, a, device(a + 1, b), device(a - 1, b),
                    lambda z, h: bufs[rnd].at[h, shard(z, b, core)],
                    lambda k: send_sem.at[rnd, 0, k], lambda k: recv_sem.at[rnd, 0, k])

    def second_ring(rnd, s):
        return Ring(n, b, device(a, b + 1), device(a, b - 1),
                    lambda z, h: bufs[rnd].at[h, shard(s, z, core)],
                    lambda k: send_sem.at[rnd, 1 + s, k], lambda k: recv_sem.at[rnd, 1 + s, k])

    def pair_copy(rnd, s, k, mine):
        if mine:
            idx = shard(s, lax.rem(b + k, n), core)
        else:
            idx = shard(s, lax.rem(a + k, n), 1 - core)
        ref = bufs[rnd].at[:, idx]
        return pltpu.make_async_remote_copy(
            src_ref=ref, dst_ref=ref, send_sem=psend_sem.at[rnd, s, k], recv_sem=precv_sem.at[rnd, s, k],
            device_id=partner, device_id_type=MESH)

    firsts = [first_ring(r) for r in range(2)]
    seconds = [[second_ring(r, s) for s in range(n)] for r in range(2)]

    def finish_second(rnd, s):
        seconds[rnd][s].finish()
        for k in range(1, n):
            pair_copy(rnd, s, k, True).start()

    def start_second(rnd, s):
        seconds[rnd][s].start()
        pair_copy(rnd, s, 0, True).start()

    def from_partner(rnd, s):
        for k in range(n):
            pair_copy(rnd, s, k, False).wait_recv()

    firsts[0].start()

    gain = gain_ref[...]
    ln_rows = 128

    def norm_rows(r):
        def body(i, carry):
            rows = pl.ds(pl.multiple_of(i * ln_rows, ln_rows), ln_rows)
            xw = x_v[r, rows, :].astype(F32)
            cen = xw - jnp.mean(xw, axis=-1, keepdims=True)
            var = jnp.mean(cen * cen, axis=-1, keepdims=True)
            h_v[r, rows, :] = (cen * lax.rsqrt(var + LN_EPS) * gain).astype(BF16)
            return carry
        lax.fori_loop(0, seq // ln_rows, body, 0)

    x_in[0].wait()
    norm_rows(0)
    firsts[0].forward()
    x_in[1].wait()
    norm_rows(1)
    firsts[0].finish()
    start_second(0, 0)
    for r in range(2, n_req):
        x_in[r].wait()
        norm_rows(r)
    seconds[0][0].forward()
    for s in range(1, n):
        start_second(0, s)
    finish_second(0, 0)
    from_partner(0, 0)

    def assemble(dst, src, rows_per, start, count):
        row = start
        while row < start + count:
            blk, r0 = row // rows_per, row % rows_per
            take = min(rows_per - r0, start + count - row)
            for h in range(2):
                dst[row - start:row - start + take, h * half:(h + 1) * half] = src[h, blk, r0:r0 + take, :]
            row += take

    assemble(wq, gi, in_rows, 0, q_width + 2 * head)

    hd2 = head // 2
    scale = float(head ** -0.5 * np.log2(np.e))
    blk = 128
    n_blk = seq // blk
    key_idx = lax.broadcasted_iota(jnp.int32, (blk, blk), 0)
    qry_idx = lax.broadcasted_iota(jnp.int32, (blk, blk), 1)

    def rotate(u):
        cos, sin = cos_ref[...], sin_ref[...]
        first, second = u[:hd2].astype(F32), u[hd2:].astype(F32)
        return jnp.concatenate([first * cos - second * sin, second * cos + first * sin], axis=0).astype(BF16)

    def scores(row, dst):
        q_rot = rotate(qkv[pl.ds(row, head), :])
        for t in range(0, seq, 2 * blk):
            stop = t + 2 * blk
            dst[:stop, t:stop] = jnp.dot(kt[:stop], q_rot[:, t:stop], preferred_element_type=F32)

    def softmax_pv(src, r):
        outs = []
        for t in range(0, n_blk, 2):
            cols, inv = [], []
            for b_q in (t, t + 1):
                lanes = slice(b_q * blk, (b_q + 1) * blk)
                diag = jnp.where(key_idx <= qry_idx, src[lanes, lanes], -1e30)
                top = jnp.max(diag, axis=0, keepdims=True)
                if b_q:
                    top = jnp.maximum(top, jnp.max(src[:b_q * blk, lanes], axis=0, keepdims=True))
                p_diag = jnp.exp2((diag - top) * scale)
                total = jnp.sum(p_diag, axis=0, keepdims=True)
                parts = [p_diag.astype(BF16)]
                if b_q:
                    p_full = jnp.exp2((src[:b_q * blk, lanes] - top) * scale)
                    total = total + jnp.sum(p_full, axis=0, keepdims=True)
                    parts.insert(0, p_full.astype(BF16))
                if b_q == t:
                    parts.append(jnp.zeros((blk, blk), BF16))
                cols.append(parts[0] if len(parts) == 1 else jnp.concatenate(parts, axis=0))
                inv.append(1.0 / total)
            probs = jnp.concatenate(cols, axis=1)
            out = jnp.dot(vc_ref[r, :, :probs.shape[0]], probs, preferred_element_type=F32)
            outs.append(out * jnp.concatenate(inv, axis=1))
        return jnp.concatenate(outs, axis=1)

    def attend(r):
        qkv[...] = nt_dot(wq[...], h_v[r]).astype(BF16)
        k_rot = rotate(qkv[q_width:q_width + head, :])
        kc_ref[r] = k_rot
        vc_ref[r] = qkv[q_width + head:, :]
        kt[...] = k_rot.astype(F32).T.astype(BF16)
        scores(0, s_a)

        def body(i, carry):
            row = pl.multiple_of(i * 2 * head, 2 * head)
            scores(row + head, s_b)
            out_a = softmax_pv(s_a, r)
            scores(jnp.minimum(row + 2 * head, q_width - head), s_a)
            out_b = softmax_pv(s_b, r)
            mixed[r, :, pl.ds(row, 2 * head)] = jnp.concatenate([out_a, out_b], axis=0).T.astype(BF16)
            return carry

        lax.fori_loop(0, q_width // (2 * head), body, 0)

    attend(0)
    seconds[0][1].forward()
    firsts[1].start()
    attend(1)
    finish_second(0, 1)
    seconds[0][2].forward()
    seconds[0][3].forward()
    attend(2)
    finish_second(0, 2)
    finish_second(0, 3)
    firsts[1].forward()
    attend(3)
    firsts[1].finish()
    for s in range(n):
        start_second(1, s)
    for s in range(1, n):
        from_partner(0, s)

    gate_at = q_width + 2 * head
    tok = 512
    tiles = seq // tok

    def mlp_chunk(c):
        assemble(wg, gi, in_rows, gate_at + c * chunk, chunk)
        assemble(wu, gi, in_rows, gate_at + ff + c * chunk, chunk)

        def body(i, carry):
            r = i // tiles
            rows = pl.ds(pl.multiple_of((i - r * tiles) * tok, tok), tok)
            h_t = h_v[r, rows, :]
            g = nt_dot(h_t, wg[...]).astype(BF16).astype(F32)
            u = nt_dot(h_t, wu[...]).astype(BF16).astype(F32)
            act = 0.5 * g * (1.0 + jnp.tanh(0.5 * g))
            mixed[r, rows, q_width + c * chunk:q_width + (c + 1) * chunk] = (act * u).astype(BF16)
            return carry
        lax.fori_loop(0, n_req * tiles, body, 0)

    for c in range(ff // chunk):
        mlp_chunk(c)
        if c < n:
            seconds[1][c].forward()
        if 1 <= c <= n:
            finish_second(1, c - 1)
    for s in range(n):
        from_partner(1, s)

    assemble(wo, go, out_rows, 0, q_width + ff)

    def y_copy(r, t):
        rows = pl.ds(pl.multiple_of(t * tok, tok), tok)
        return pltpu.make_async_copy(x_v.at[r, rows], y_hbm.at[r, rows], y_sem.at[r, t])

    def out_body(i, carry):
        r = i // tiles
        t = i - r * tiles
        rows = pl.ds(pl.multiple_of(t * tok, tok), tok)
        acc = jnp.dot(mixed[r, rows, :], wo[...], preferred_element_type=F32)
        x_v[r, rows, :] = (x_v[r, rows, :].astype(F32) + acc).astype(BF16)
        y_copy(r, t).start()
        return carry
    lax.fori_loop(0, n_req * tiles, out_body, 0)

    for r in range(n_req):
        for t in range(tiles):
            y_copy(r, t).wait()
    for rnd in range(2):
        firsts[rnd].drain()
        for s in range(n):
            seconds[rnd][s].drain()
            for k in range(n):
                pair_copy(rnd, s, k, True).wait_send()


def rope_tables(seq, head):
    inv_freq = (np.float32(ROPE_BASE) ** (-np.arange(head // 2, dtype=np.float32) * np.float32(2.0) / np.float32(head)))
    angles = inv_freq.astype(np.float32)[:, None] * np.arange(seq, dtype=np.float32)[None, :]
    return np.cos(angles).astype(np.float32), np.sin(angles).astype(np.float32)


def solution(mesh):
    tok_spec = P(('part', 'dp', 'tp'))
    n = mesh.shape['tp']
    n_dev = n * mesh.shape['dp']

    def per_device(x_blk, ln_gain, w_in_blk, w_out_blk):
        n_req, seq, d = x_blk.shape
        in_rows, out_rows = w_in_blk.shape[1], w_out_blk.shape[0]
        ff = 4 * d
        q_width = out_rows * n_dev - ff
        head = (in_rows * n_dev - q_width - 2 * ff) // 2
        chunk = min(512, ff)
        cos, sin = rope_tables(seq, head)
        vmem = pl.BlockSpec(memory_space=pltpu.VMEM)
        anyw = pl.BlockSpec(memory_space=pl.ANY)
        tiles = seq // 512
        y, kc, vc = pl.pallas_call(
            functools.partial(layer_kernel, n),
            out_shape=(jax.ShapeDtypeStruct(x_blk.shape, BF16),
                       jax.ShapeDtypeStruct((n_req, head, seq), BF16),
                       jax.ShapeDtypeStruct((n_req, head, seq), BF16)),
            in_specs=[anyw, vmem, anyw, anyw, vmem, vmem],
            out_specs=(anyw, vmem, vmem),
            scratch_shapes=[
                pltpu.VMEM((n_req, seq, d), BF16),
                pltpu.VMEM((n_req, seq, d), BF16),
                pltpu.VMEM((n_req, seq, q_width + ff), BF16),
                pltpu.VMEM((2, n_dev, in_rows, d // 2), BF16),
                pltpu.VMEM((2, n_dev, out_rows, d // 2), BF16),
                pltpu.VMEM((q_width + 2 * head, d), BF16),
                pltpu.VMEM((chunk, d), BF16),
                pltpu.VMEM((chunk, d), BF16),
                pltpu.VMEM((q_width + ff, d), BF16),
                pltpu.VMEM((q_width + 2 * head, seq), BF16),
                pltpu.VMEM((seq, head), BF16),
                pltpu.VMEM((seq, seq), F32),
                pltpu.VMEM((seq, seq), F32),
                pltpu.SemaphoreType.DMA((n_req,)),
                pltpu.SemaphoreType.DMA((2, 2)),
                pltpu.SemaphoreType.DMA((n_req, tiles)),
                pltpu.SemaphoreType.DMA((2, 1 + n, 6)),
                pltpu.SemaphoreType.DMA((2, 1 + n, 6)),
                pltpu.SemaphoreType.DMA((2, n, n)),
                pltpu.SemaphoreType.DMA((2, n, n)),
            ],
            compiler_params=pltpu.CompilerParams(
                collective_id=0, has_side_effects=True, vmem_limit_bytes=63 * 1024 * 1024),
        )(x_blk, ln_gain.reshape(1, d), w_in_blk.T, w_out_blk, cos, sin)
        return y, kc.swapaxes(1, 2), vc.swapaxes(1, 2)

    return jax.shard_map(per_device, mesh=mesh,
                         in_specs=(tok_spec, P(), P(None, ('dp', 'tp')), P(('dp', 'tp'), None)),
                         out_specs=(tok_spec, tok_spec, tok_spec), check_vma=False)
```

```python
import functools

import jax
import jax.numpy as jnp
import numpy as np
from jax import lax
from jax.experimental import pallas as pl
from jax.experimental.pallas import tpu as pltpu
from jax.sharding import PartitionSpec as P

LN_EPS = 1e-6
ROPE_BASE = 10000.0
MESH = pl.DeviceIdType.MESH
F32 = jnp.float32
BF16 = jnp.bfloat16


def nt_dot(lhs, rhs):
    return lax.dot_general(lhs, rhs, (((1,), (1,)), ((), ())), preferred_element_type=F32)


class Ring:
    def __init__(self, n, pos, right, left, block, send, recv):
        self.n, self.pos, self.right, self.left = n, pos, right, left
        self.block, self.send, self.recv = block, send, recv
        self.routes = ((0, 0, True), (0, 1, True), (1, 0, True), (0, 1, False), (0, 0, False), (1, 1, False))

    def _copy(self, k, hops):
        back, half, to_right = self.routes[k]
        step = (back + hops) if to_right else self.n - (back + hops)
        z = lax.rem(self.pos - step + 2 * self.n, self.n)
        ref = self.block(z, half)
        return pltpu.make_async_remote_copy(
            src_ref=ref, dst_ref=ref, send_sem=self.send(k), recv_sem=self.recv(k),
            device_id=self.right if to_right else self.left, device_id_type=MESH)

    def start(self):
        for k in (0, 3, 1, 4):
            self._copy(k, 0).start()

    def forward(self):
        self._copy(0, 1).wait_recv()
        self._copy(2, 0).start()
        self._copy(3, 1).wait_recv()
        self._copy(5, 0).start()

    def finish(self):
        for k in (1, 4, 2, 5):
            self._copy(k, 1).wait_recv()

    def drain(self):
        for k in range(6):
            self._copy(k, 0).wait_send()


def layer_kernel(n, x_hbm, gain_ref, wi_hbm, wo_hbm, cos_ref, sin_ref, y_hbm, kc_ref, vc_ref,
                 x_v, h_v, mixed, gi, go, wq, wg, wu, wo, qkv, kt, s_a, s_b,
                 x_sem, own_sem, y_sem, send_sem, recv_sem, psend_sem, precv_sem, qsend_sem, qrecv_sem):
    n_req, seq, d = x_v.shape
    parts, _, in_rows, lanes = gi.shape
    out_rows, half = go.shape[2], go.shape[3]
    mid = parts // 2
    n_dev = gi.shape[1]
    head = kc_ref.shape[1]
    q_width = wq.shape[0] - 2 * head
    ff = wo.shape[0] - q_width
    chunk = wg.shape[0]

    dp, tp = lax.axis_index("dp"), lax.axis_index("tp")
    core, x, y = lax.rem(dp, 2), dp // 2, tp
    a = (1 - core) * x + core * y
    b = (1 - core) * y + core * x

    def place(za, zb, c):
        zx = (1 - c) * za + c * zb
        zy = (1 - c) * zb + c * za
        return zx * 2 + c, zy

    def device(za, zb):
        zdp, ztp = place(lax.rem(za + n, n), lax.rem(zb + n, n), core)
        return {"dp": zdp, "tp": ztp}

    def shard(za, zb, c):
        zdp, ztp = place(za, zb, c)
        return zdp * n + ztp

    partner = {"dp": x * 2 + 1 - core, "tp": tp}
    bufs = (gi, go)
    me = dp * n + tp

    own = []
    for p in range(parts):
        own.append(pltpu.make_async_copy(wi_hbm.at[:, pl.ds(p * lanes, lanes)], gi.at[p, me], own_sem.at[p]))
    for h in range(2):
        own.append(pltpu.make_async_copy(wo_hbm.at[:, pl.ds(h * half, half)], go.at[h, me], own_sem.at[parts + h]))
    for copy in own:
        copy.start()
    x_in = [pltpu.make_async_copy(x_hbm.at[r], x_v.at[r], x_sem.at[r]) for r in range(n_req)]
    for copy in x_in:
        copy.start()

    barrier = pltpu.get_barrier_semaphore()
    for dev in (device(a + 1, b), device(a - 1, b), device(a, b + 1), device(a, b - 1), partner):
        pl.semaphore_signal(barrier, inc=1, device_id=dev, device_id_type=MESH)
    pl.semaphore_wait(barrier, 5)
    for copy in own:
        copy.wait()

    def piece(rnd, h, idx):
        return gi.at[pl.ds(h * mid, mid), idx] if rnd == 0 else go.at[h, idx]

    def first_ring(rnd):
        return Ring(n, a, device(a + 1, b), device(a - 1, b),
                    lambda z, h: piece(rnd, h, shard(z, b, core)),
                    lambda k: send_sem.at[rnd, 0, k], lambda k: recv_sem.at[rnd, 0, k])

    def second_ring(rnd, s):
        return Ring(n, b, device(a, b + 1), device(a, b - 1),
                    lambda z, h: piece(rnd, h, shard(s, z, core)),
                    lambda k: send_sem.at[rnd, 1 + s, k], lambda k: recv_sem.at[rnd, 1 + s, k])

    def pair_copy(rnd, s, k, mine):
        if mine:
            idx = shard(s, lax.rem(b + k, n), core)
        else:
            idx = shard(s, lax.rem(a + k, n), 1 - core)
        ref = bufs[rnd].at[:, idx]
        return pltpu.make_async_remote_copy(
            src_ref=ref, dst_ref=ref, send_sem=psend_sem.at[rnd, s, k], recv_sem=precv_sem.at[rnd, s, k],
            device_id=partner, device_id_type=MESH)

    last = first_ring(1)

    def finish_second(rnd, s):
        second_ring(rnd, s).finish()
        for k in range(1, n):
            pair_copy(rnd, s, k, True).start()

    def start_second(rnd, s):
        second_ring(rnd, s).start()
        pair_copy(rnd, s, 0, True).start()

    def from_partner(rnd, s):
        for k in range(n):
            pair_copy(rnd, s, k, False).wait_recv()

    RIGHT, LEFT = 0, 1
    to_right, to_left = range(mid), range(mid, parts)

    def piece_copy(stage, way, p, back, arriving=False):
        step = back + (1 if arriving else 0)
        pos = b if stage else a
        z = lax.rem(pos + n - step, n) if way == RIGHT else lax.rem(pos + step, n)
        ref = gi.at[p, shard(0, z, core) if stage else shard(z, b, core)]
        sem = p if back == 0 else parts + (p if way == RIGHT else p - mid)
        sign = 1 if way == RIGHT else -1
        return pltpu.make_async_remote_copy(
            src_ref=ref, dst_ref=ref, send_sem=qsend_sem.at[stage, way, sem], recv_sem=qrecv_sem.at[stage, way, sem],
            device_id=device(a, b + sign) if stage else device(a + sign, b), device_id_type=MESH)

    def send(stage, way, p, back=0):
        piece_copy(stage, way, p, back).start()

    def arrive(stage, way, p, back=0):
        piece_copy(stage, way, p, back, True).wait_recv()

    def own_all(way):
        for p in (*to_right, *to_left) if way == RIGHT else (*to_left, *to_right):
            send(0, way, p)

    def forward_all(way):
        for p in to_right if way == RIGHT else to_left:
            arrive(0, way, p)
            send(0, way, p, 1)

    def pass_on(way, p):
        arrive(1, way, p)
        send(1, way, p, 1)

    def first_step(role, i):
        mixed_order = tuple(p for pair in zip(to_right, to_left) for p in pair)
        order = {1: (*to_right, *to_left), n - 1: (*to_left, *to_right)}.get(role, mixed_order)
        p = order[i]
        if role == 1:
            arrive(0, RIGHT, p)
            if p in to_right:
                send(0, RIGHT, p, 1)
        elif role == n - 1:
            arrive(0, LEFT, p)
            if p in to_left:
                send(0, LEFT, p, 1)
        elif role:
            arrive(0, RIGHT if p in to_right else LEFT, p, 1)
        send(1, RIGHT, p)
        send(1, LEFT, p)
        if role == 1 and i == mid - 1:
            own_all(RIGHT)
        if role == n - 1 and i == mid - 1:
            own_all(LEFT)
        if i >= mid:
            if role == 1:
                pass_on(RIGHT, i - mid)
            elif role == n - 1:
                pass_on(LEFT, i)
            elif i == mid:
                pass_on(RIGHT, 0)
                pass_on(LEFT, mid)
            elif i == parts - 1:
                for j in range(1, mid):
                    pass_on(RIGHT, j)
                    pass_on(LEFT, mid + j)

    def on_role(role, fn):
        pl.when(a == role)(fn)

    on_role(0, lambda: (own_all(RIGHT), own_all(LEFT)) and None)
    on_role(1, lambda: own_all(LEFT))
    on_role(n - 1, lambda: own_all(RIGHT))
    on_role(2, lambda: (own_all(RIGHT), own_all(LEFT)) and None)

    gain = gain_ref[...].reshape(1, d)
    ln_rows = 128
    per_req = seq // ln_rows

    def norm_rows(first, count):
        def body(i, carry):
            j = first + i
            r = j // per_req
            rows = pl.ds(pl.multiple_of((j - r * per_req) * ln_rows, ln_rows), ln_rows)
            xw = x_v[r, rows, :].astype(F32)
            cen = xw - jnp.mean(xw, axis=-1, keepdims=True)
            var = jnp.mean(cen * cen, axis=-1, keepdims=True)
            h_v[r, rows, :] = (cen * lax.rsqrt(var + LN_EPS) * gain).astype(BF16)
            return carry
        lax.fori_loop(0, count, body, 0)

    for copy in x_in:
        copy.wait()
    blocks = n_req * per_req
    share = blocks // (parts + 2)
    norm_rows(0, blocks - share * parts)
    for i in range(parts):
        for role in range(n):
            on_role(role, functools.partial(first_step, role, i))
        norm_rows(blocks - share * (parts - i), share)
    pair_copy(0, 0, 0, True).start()
    on_role(1, lambda: [pass_on(LEFT, p) for p in to_left] and None)
    on_role(n - 1, lambda: [pass_on(RIGHT, p) for p in to_right] and None)
    for p in to_left:
        arrive(1, RIGHT, p)
    pair_copy(0, 0, n - 1, True).start()
    for p in to_right:
        arrive(1, LEFT, p)
    pair_copy(0, 0, 1, True).start()
    for p in to_right:
        arrive(1, RIGHT, p, 1)
    for p in to_left:
        arrive(1, LEFT, p, 1)
    pair_copy(0, 0, 2, True).start()

    pl.when(a != 1)(lambda: forward_all(RIGHT))
    pl.when(a != n - 1)(lambda: forward_all(LEFT))

    @pl.when(a != 1)
    def _():
        for p in to_left:
            arrive(0, RIGHT, p)

    @pl.when(a != n - 1)
    def _():
        for p in to_right:
            arrive(0, LEFT, p)

    def later(k, fn):
        s = lax.rem(a + k, n)
        pl.when(s != 0)(lambda: fn(0, s))

    def far_arrivals(rnd, s):
        for p in to_right:
            arrive(0, RIGHT, p, 1)
        for p in to_left:
            arrive(0, LEFT, p, 1)
        start_second(rnd, s)

    def forward_second(rnd, s):
        second_ring(rnd, s).forward()

    for k in (0, 1, 3):
        later(k, start_second)
    from_partner(0, 0)

    def assemble(dst, src, rows_per, start, count):
        row = start
        while row < start + count:
            blk, r0 = row // rows_per, row % rows_per
            take = min(rows_per - r0, start + count - row)
            width = src.shape[3]
            for h in range(src.shape[0]):
                dst[row - start:row - start + take, h * width:(h + 1) * width] = src[h, blk, r0:r0 + take, :]
            row += take

    assemble(wq, gi, in_rows, 0, q_width + 2 * head)

    hd2 = head // 2
    scale = float(head ** -0.5 * np.log2(np.e))
    blk = 128
    n_blk = seq // blk
    key_idx = lax.broadcasted_iota(jnp.int32, (blk, blk), 0)
    qry_idx = lax.broadcasted_iota(jnp.int32, (blk, blk), 1)

    def rotate(u):
        cos, sin = cos_ref[...], sin_ref[...]
        first, second = u[:hd2].astype(F32), u[hd2:].astype(F32)
        return jnp.concatenate([first * cos - second * sin, second * cos + first * sin], axis=0).astype(BF16)

    def scores(row, dst):
        q_rot = rotate(qkv[pl.ds(row, head), :])
        for t in range(0, seq, 2 * blk):
            stop = t + 2 * blk
            dst[:stop, t:stop] = jnp.dot(kt[:stop], q_rot[:, t:stop], preferred_element_type=F32)

    def softmax_pv(src, r):
        outs = []
        for t in range(0, n_blk, 2):
            cols, inv = [], []
            for b_q in (t, t + 1):
                lanes = slice(b_q * blk, (b_q + 1) * blk)
                diag = jnp.where(key_idx <= qry_idx, src[lanes, lanes], -1e30)
                top = jnp.max(diag, axis=0, keepdims=True)
                if b_q:
                    top = jnp.maximum(top, jnp.max(src[:b_q * blk, lanes], axis=0, keepdims=True))
                p_diag = jnp.exp2((diag - top) * scale)
                total = jnp.sum(p_diag, axis=0, keepdims=True)
                parts = [p_diag.astype(BF16)]
                if b_q:
                    p_full = jnp.exp2((src[:b_q * blk, lanes] - top) * scale)
                    total = total + jnp.sum(p_full, axis=0, keepdims=True)
                    parts.insert(0, p_full.astype(BF16))
                if b_q == t:
                    parts.append(jnp.zeros((blk, blk), BF16))
                cols.append(parts[0] if len(parts) == 1 else jnp.concatenate(parts, axis=0))
                inv.append(1.0 / total)
            probs = jnp.concatenate(cols, axis=1)
            out = jnp.dot(vc_ref[r, :, :probs.shape[0]], probs, preferred_element_type=F32)
            outs.append(out * jnp.concatenate(inv, axis=1))
        return jnp.concatenate(outs, axis=1)

    def attend(r, between, after):
        qkv[...] = nt_dot(wq[...], h_v[r]).astype(BF16)
        k_rot = rotate(qkv[q_width:q_width + head, :])
        kc_ref[r] = k_rot
        vc_ref[r] = qkv[q_width + head:, :]
        kt[...] = k_rot.astype(F32).T.astype(BF16)
        scores(0, s_a)

        def body(i, carry):
            row = pl.multiple_of(i * 2 * head, 2 * head)
            scores(row + head, s_b)
            out_a = softmax_pv(s_a, r)
            scores(jnp.minimum(row + 2 * head, q_width - head), s_a)
            out_b = softmax_pv(s_b, r)
            mixed[r, :, pl.ds(row, 2 * head)] = jnp.concatenate([out_a, out_b], axis=0).T.astype(BF16)
            return carry

        pairs = q_width // (2 * head)
        lax.fori_loop(0, pairs // 2, body, 0)
        between()
        lax.fori_loop(pairs // 2, pairs, body, 0)
        after()

    def slot(*todo):
        def run():
            for k, fn in todo:
                later(k, fn)
        return run

    attend(0, slot(), slot((0, forward_second), (2, far_arrivals)))
    attend(1, slot((1, forward_second)), slot((0, finish_second)))
    attend(2, slot((3, forward_second), (1, finish_second)), slot((2, forward_second)))
    last.start()
    attend(3, slot((3, finish_second)), slot((2, finish_second)))
    last.forward()
    for s in range(1, n):
        from_partner(0, s)

    gate_at = q_width + 2 * head
    tok = 512
    tiles = seq // tok

    def mlp_chunk(c):
        assemble(wg, gi, in_rows, gate_at + c * chunk, chunk)
        assemble(wu, gi, in_rows, gate_at + ff + c * chunk, chunk)

        def body(i, carry):
            r = i // tiles
            rows = pl.ds(pl.multiple_of((i - r * tiles) * tok, tok), tok)
            h_t = h_v[r, rows, :]
            g = nt_dot(h_t, wg[...]).astype(BF16).astype(F32)
            u = nt_dot(h_t, wu[...]).astype(BF16).astype(F32)
            act = 0.5 * g * (1.0 + jnp.tanh(0.5 * g))
            mixed[r, rows, q_width + c * chunk:q_width + (c + 1) * chunk] = (act * u).astype(BF16)
            return carry
        lax.fori_loop(0, n_req * tiles, body, 0)

    for c in range(ff // chunk):
        mlp_chunk(c)
        if c == 0:
            last.finish()
            for s in range(n):
                start_second(1, s)
        if c == 1:
            forward_second(1, 0)
            forward_second(1, 1)
        if c == 2:
            forward_second(1, 2)
            forward_second(1, 3)
            finish_second(1, 0)
            finish_second(1, 1)
        if c == 3:
            finish_second(1, 2)
            finish_second(1, 3)
    for s in range(n):
        from_partner(1, s)

    assemble(wo, go, out_rows, 0, q_width + ff)

    def y_copy(r, t):
        rows = pl.ds(pl.multiple_of(t * tok, tok), tok)
        return pltpu.make_async_copy(x_v.at[r, rows], y_hbm.at[r, rows], y_sem.at[r, t])

    def out_body(i, carry):
        r = i // tiles
        t = i - r * tiles
        rows = pl.ds(pl.multiple_of(t * tok, tok), tok)
        acc = jnp.dot(mixed[r, rows, :], wo[...], preferred_element_type=F32)
        x_v[r, rows, :] = (x_v[r, rows, :].astype(F32) + acc).astype(BF16)
        y_copy(r, t).start()
        return carry
    lax.fori_loop(0, n_req * tiles, out_body, 0)

    for r in range(n_req):
        for t in range(tiles):
            y_copy(r, t).wait()
    for stage in range(2):
        for way in (RIGHT, LEFT):
            for p in range(parts):
                piece_copy(stage, way, p, 0).wait_send()
            for p in to_right if way == RIGHT else to_left:
                piece_copy(stage, way, p, 1).wait_send()
    last.drain()
    for rnd in range(2):
        for s in range(n):
            if rnd or s:
                second_ring(rnd, s).drain()
            for k in range(n):
                pair_copy(rnd, s, k, True).wait_send()


def rope_tables(seq, head):
    inv_freq = (np.float32(ROPE_BASE) ** (-np.arange(head // 2, dtype=np.float32) * np.float32(2.0) / np.float32(head)))
    angles = inv_freq.astype(np.float32)[:, None] * np.arange(seq, dtype=np.float32)[None, :]
    return np.cos(angles).astype(np.float32), np.sin(angles).astype(np.float32)


def solution(mesh):
    tok_spec = P(('part', 'dp', 'tp'))
    n = mesh.shape['tp']
    n_dev = n * mesh.shape['dp']

    def per_device(x_blk, ln_gain, w_in_blk, w_out_blk):
        n_req, seq, d = x_blk.shape
        in_rows, out_rows = w_in_blk.shape[1], w_out_blk.shape[0]
        ff = 4 * d
        q_width = out_rows * n_dev - ff
        head = (in_rows * n_dev - q_width - 2 * ff) // 2
        chunk = min(512, ff)
        parts = d // 128
        cos, sin = rope_tables(seq, head)
        vmem = pl.BlockSpec(memory_space=pltpu.VMEM)
        anyw = pl.BlockSpec(memory_space=pl.ANY)
        tiles = seq // 512
        y, kc, vc = pl.pallas_call(
            functools.partial(layer_kernel, n),
            out_shape=(jax.ShapeDtypeStruct(x_blk.shape, BF16),
                       jax.ShapeDtypeStruct((n_req, head, seq), BF16),
                       jax.ShapeDtypeStruct((n_req, head, seq), BF16)),
            in_specs=[anyw, vmem, anyw, anyw, vmem, vmem],
            out_specs=(anyw, vmem, vmem),
            scratch_shapes=[
                pltpu.VMEM((n_req, seq, d), BF16),
                pltpu.VMEM((n_req, seq, d), BF16),
                pltpu.VMEM((n_req, seq, q_width + ff), BF16),
                pltpu.VMEM((parts, n_dev, in_rows, d // parts), BF16),
                pltpu.VMEM((2, n_dev, out_rows, d // 2), BF16),
                pltpu.VMEM((q_width + 2 * head, d), BF16),
                pltpu.VMEM((chunk, d), BF16),
                pltpu.VMEM((chunk, d), BF16),
                pltpu.VMEM((q_width + ff, d), BF16),
                pltpu.VMEM((q_width + 2 * head, seq), BF16),
                pltpu.VMEM((seq, head), BF16),
                pltpu.VMEM((seq, seq), F32),
                pltpu.VMEM((seq, seq), F32),
                pltpu.SemaphoreType.DMA((n_req,)),
                pltpu.SemaphoreType.DMA((parts + 2,)),
                pltpu.SemaphoreType.DMA((n_req, tiles)),
                pltpu.SemaphoreType.DMA((2, 1 + n, 6)),
                pltpu.SemaphoreType.DMA((2, 1 + n, 6)),
                pltpu.SemaphoreType.DMA((2, n, n)),
                pltpu.SemaphoreType.DMA((2, n, n)),
                pltpu.SemaphoreType.DMA((2, 2, parts + parts // 2)),
                pltpu.SemaphoreType.DMA((2, 2, parts + parts // 2)),
            ],
            compiler_params=pltpu.CompilerParams(
                collective_id=0, has_side_effects=True, vmem_limit_bytes=63 * 1024 * 1024),
        )(x_blk, ln_gain, w_in_blk.T, w_out_blk, cos, sin)
        return y, kc.swapaxes(1, 2), vc.swapaxes(1, 2)

    return jax.shard_map(per_device, mesh=mesh,
                         in_specs=(tok_spec, P(), P(None, ('dp', 'tp')), P(('dp', 'tp'), None)),
                         out_specs=(tok_spec, tok_spec, tok_spec), check_vma=False)
```

```python
import functools

import jax
import jax.numpy as jnp
import numpy as np
from jax import lax
from jax.experimental import pallas as pl
from jax.experimental.pallas import tpu as pltpu
from jax.sharding import PartitionSpec as P

LN_EPS = 1e-6
ROPE_BASE = 10000.0
MESH = pl.DeviceIdType.MESH
F32 = jnp.float32
BF16 = jnp.bfloat16


def nt_dot(lhs, rhs):
    return lax.dot_general(lhs, rhs, (((1,), (1,)), ((), ())), preferred_element_type=F32)


class Ring:
    def __init__(self, n, pos, right, left, block, send, recv):
        self.n, self.pos, self.right, self.left = n, pos, right, left
        self.block, self.send, self.recv = block, send, recv
        self.routes = ((0, 0, True), (0, 1, True), (1, 0, True), (0, 1, False), (0, 0, False), (1, 1, False))

    def _copy(self, k, hops):
        back, half, to_right = self.routes[k]
        step = (back + hops) if to_right else self.n - (back + hops)
        z = lax.rem(self.pos - step + 2 * self.n, self.n)
        ref = self.block(z, half)
        return pltpu.make_async_remote_copy(
            src_ref=ref, dst_ref=ref, send_sem=self.send(k), recv_sem=self.recv(k),
            device_id=self.right if to_right else self.left, device_id_type=MESH)

    def start(self):
        for k in (0, 3, 1, 4):
            self._copy(k, 0).start()

    def forward(self):
        self._copy(0, 1).wait_recv()
        self._copy(2, 0).start()
        self._copy(3, 1).wait_recv()
        self._copy(5, 0).start()

    def finish(self):
        for k in (1, 4, 2, 5):
            self._copy(k, 1).wait_recv()

    def drain(self):
        for k in range(6):
            self._copy(k, 0).wait_send()


def layer_kernel(n, x_hbm, gain_ref, wi_hbm, wo_hbm, cos_ref, sin_ref, y_hbm, kc_ref, vc_ref,
                 x_v, h_v, mixed, gi, go, wq, wg, wu, wo, qkv, kt, s_a, s_b,
                 x_sem, own_sem, y_sem, send_sem, recv_sem, psend_sem, precv_sem, qsend_sem, qrecv_sem):
    n_req, seq, d = x_v.shape
    parts, _, in_rows, lanes = gi.shape
    out_rows, half = go.shape[2], go.shape[3]
    mid = parts // 2
    n_dev = gi.shape[1]
    head = kc_ref.shape[1]
    q_width = wq.shape[0] - 2 * head
    ff = wo.shape[0] - q_width
    chunk = wg.shape[0]

    dp, tp = lax.axis_index("dp"), lax.axis_index("tp")
    core, x, y = lax.rem(dp, 2), dp // 2, tp
    a = (1 - core) * x + core * y
    b = (1 - core) * y + core * x

    def place(za, zb, c):
        zx = (1 - c) * za + c * zb
        zy = (1 - c) * zb + c * za
        return zx * 2 + c, zy

    def device(za, zb):
        zdp, ztp = place(lax.rem(za + n, n), lax.rem(zb + n, n), core)
        return {"dp": zdp, "tp": ztp}

    def shard(za, zb, c):
        zdp, ztp = place(za, zb, c)
        return zdp * n + ztp

    partner = {"dp": x * 2 + 1 - core, "tp": tp}
    bufs = (gi, go)
    me = dp * n + tp

    own = []
    for p in range(parts):
        own.append(pltpu.make_async_copy(wi_hbm.at[:, pl.ds(p * lanes, lanes)], gi.at[p, me], own_sem.at[p]))
    for h in range(2):
        own.append(pltpu.make_async_copy(wo_hbm.at[:, pl.ds(h * half, half)], go.at[h, me], own_sem.at[parts + h]))
    for copy in own:
        copy.start()
    x_in = [pltpu.make_async_copy(x_hbm.at[r], x_v.at[r], x_sem.at[r]) for r in range(n_req)]
    for copy in x_in:
        copy.start()

    barrier = pltpu.get_barrier_semaphore()
    for dev in (device(a + 1, b), device(a - 1, b), device(a, b + 1), device(a, b - 1), partner):
        pl.semaphore_signal(barrier, inc=1, device_id=dev, device_id_type=MESH)
    pl.semaphore_wait(barrier, 5)
    for copy in own:
        copy.wait()

    def piece(rnd, h, idx):
        return gi.at[pl.ds(h * mid, mid), idx] if rnd == 0 else go.at[h, idx]

    def first_ring(rnd):
        return Ring(n, a, device(a + 1, b), device(a - 1, b),
                    lambda z, h: piece(rnd, h, shard(z, b, core)),
                    lambda k: send_sem.at[rnd, 0, k], lambda k: recv_sem.at[rnd, 0, k])

    def second_ring(rnd, s):
        return Ring(n, b, device(a, b + 1), device(a, b - 1),
                    lambda z, h: piece(rnd, h, shard(s, z, core)),
                    lambda k: send_sem.at[rnd, 1 + s, k], lambda k: recv_sem.at[rnd, 1 + s, k])

    def pair_copy(rnd, s, k, mine):
        if mine:
            idx = shard(s, lax.rem(b + k, n), core)
        else:
            idx = shard(s, lax.rem(a + k, n), 1 - core)
        ref = bufs[rnd].at[:, idx]
        return pltpu.make_async_remote_copy(
            src_ref=ref, dst_ref=ref, send_sem=psend_sem.at[rnd, s, k], recv_sem=precv_sem.at[rnd, s, k],
            device_id=partner, device_id_type=MESH)

    last = first_ring(1)

    def finish_second(rnd, s):
        second_ring(rnd, s).finish()
        for k in range(1, n):
            pair_copy(rnd, s, k, True).start()

    def start_second(rnd, s):
        second_ring(rnd, s).start()
        pair_copy(rnd, s, 0, True).start()

    def from_partner(rnd, s):
        for k in range(n):
            pair_copy(rnd, s, k, False).wait_recv()

    RIGHT, LEFT = 0, 1
    to_right, to_left = range(mid), range(mid, parts)

    def piece_copy(stage, way, p, back, arriving=False):
        step = back + (1 if arriving else 0)
        pos = b if stage else a
        z = lax.rem(pos + n - step, n) if way == RIGHT else lax.rem(pos + step, n)
        ref = gi.at[p, shard(0, z, core) if stage else shard(z, b, core)]
        sem = p if back == 0 else parts + (p if way == RIGHT else p - mid)
        sign = 1 if way == RIGHT else -1
        return pltpu.make_async_remote_copy(
            src_ref=ref, dst_ref=ref, send_sem=qsend_sem.at[stage, way, sem], recv_sem=qrecv_sem.at[stage, way, sem],
            device_id=device(a, b + sign) if stage else device(a + sign, b), device_id_type=MESH)

    def send(stage, way, p, back=0):
        piece_copy(stage, way, p, back).start()

    def arrive(stage, way, p, back=0):
        piece_copy(stage, way, p, back, True).wait_recv()

    def own_all(way):
        for p in (*to_right, *to_left) if way == RIGHT else (*to_left, *to_right):
            send(0, way, p)

    def forward_all(way):
        for p in to_right if way == RIGHT else to_left:
            arrive(0, way, p)
            send(0, way, p, 1)

    def pass_on(way, p):
        arrive(1, way, p)
        send(1, way, p, 1)

    def first_step(role, i):
        mixed_order = tuple(p for pair in zip(to_right, to_left) for p in pair)
        order = {1: (*to_right, *to_left), n - 1: (*to_left, *to_right)}.get(role, mixed_order)
        p = order[i]
        if role == 1:
            arrive(0, RIGHT, p)
            if p in to_right:
                send(0, RIGHT, p, 1)
        elif role == n - 1:
            arrive(0, LEFT, p)
            if p in to_left:
                send(0, LEFT, p, 1)
        elif role:
            arrive(0, RIGHT if p in to_right else LEFT, p, 1)
        send(1, RIGHT, p)
        send(1, LEFT, p)
        if role == 1 and i == mid - 1:
            own_all(RIGHT)
        if role == n - 1 and i == mid - 1:
            own_all(LEFT)
        if i >= mid:
            if role == 1:
                pass_on(RIGHT, i - mid)
            elif role == n - 1:
                pass_on(LEFT, i)
            elif i == mid:
                pass_on(RIGHT, 0)
                pass_on(LEFT, mid)
            elif i == parts - 1:
                for j in range(1, mid):
                    pass_on(RIGHT, j)
                    pass_on(LEFT, mid + j)

    def on_role(role, fn):
        pl.when(a == role)(fn)

    on_role(0, lambda: (own_all(RIGHT), own_all(LEFT)) and None)
    on_role(1, lambda: own_all(LEFT))
    on_role(n - 1, lambda: own_all(RIGHT))
    on_role(2, lambda: (own_all(RIGHT), own_all(LEFT)) and None)

    gain = gain_ref[...].reshape(1, d)
    ln_rows = 128
    per_req = seq // ln_rows

    def norm_rows(first, count):
        def body(i, carry):
            j = first + i
            r = j // per_req
            rows = pl.ds(pl.multiple_of((j - r * per_req) * ln_rows, ln_rows), ln_rows)
            xw = x_v[r, rows, :].astype(F32)
            cen = xw - jnp.mean(xw, axis=-1, keepdims=True)
            var = jnp.mean(cen * cen, axis=-1, keepdims=True)
            h_v[r, rows, :] = (cen * lax.rsqrt(var + LN_EPS) * gain).astype(BF16)
            return carry
        lax.fori_loop(0, count, body, 0)

    for copy in x_in:
        copy.wait()
    blocks = n_req * per_req
    share = blocks // (parts + 2)
    norm_rows(0, blocks - share * parts)
    for i in range(parts):
        for role in range(n):
            on_role(role, functools.partial(first_step, role, i))
        norm_rows(blocks - share * (parts - i), share)
    pair_copy(0, 0, 0, True).start()
    on_role(1, lambda: [pass_on(LEFT, p) for p in to_left] and None)
    on_role(n - 1, lambda: [pass_on(RIGHT, p) for p in to_right] and None)
    for p in to_left:
        arrive(1, RIGHT, p)
    pair_copy(0, 0, n - 1, True).start()
    for p in to_right:
        arrive(1, LEFT, p)
    pair_copy(0, 0, 1, True).start()
    for p in to_right:
        arrive(1, RIGHT, p, 1)
    for p in to_left:
        arrive(1, LEFT, p, 1)
    pair_copy(0, 0, 2, True).start()

    pl.when(a != 1)(lambda: forward_all(RIGHT))
    pl.when(a != n - 1)(lambda: forward_all(LEFT))

    @pl.when(a != 1)
    def _():
        for p in to_left:
            arrive(0, RIGHT, p)

    @pl.when(a != n - 1)
    def _():
        for p in to_right:
            arrive(0, LEFT, p)

    def far_arrivals():
        for p in to_right:
            arrive(0, RIGHT, p, 1)
        for p in to_left:
            arrive(0, LEFT, p, 1)

    def forward_second(rnd, s):
        second_ring(rnd, s).forward()

    step_a = 1 + a // (n - 1)
    step_b = 3 - step_a
    start_second(0, step_a)
    from_partner(0, 0)

    def assemble(dst, src, rows_per, start, count):
        row = start
        while row < start + count:
            blk, r0 = row // rows_per, row % rows_per
            take = min(rows_per - r0, start + count - row)
            width = src.shape[3]
            for h in range(src.shape[0]):
                dst[row - start:row - start + take, h * width:(h + 1) * width] = src[h, blk, r0:r0 + take, :]
            row += take

    assemble(wq, gi, in_rows, 0, q_width + 2 * head)

    hd2 = head // 2
    scale = float(head ** -0.5 * np.log2(np.e))
    blk = 128
    n_blk = seq // blk
    key_idx = lax.broadcasted_iota(jnp.int32, (blk, blk), 0)
    qry_idx = lax.broadcasted_iota(jnp.int32, (blk, blk), 1)

    def rotate(u):
        cos, sin = cos_ref[...], sin_ref[...]
        first, second = u[:hd2].astype(F32), u[hd2:].astype(F32)
        return jnp.concatenate([first * cos - second * sin, second * cos + first * sin], axis=0).astype(BF16)

    def scores(row, dst):
        q_rot = rotate(qkv[pl.ds(row, head), :])
        for t in range(0, seq, 2 * blk):
            stop = t + 2 * blk
            dst[:stop, t:stop] = jnp.dot(kt[:stop], q_rot[:, t:stop], preferred_element_type=F32)

    def softmax_pv(src, r):
        outs = []
        for t in range(0, n_blk, 2):
            cols, inv = [], []
            for b_q in (t, t + 1):
                lanes = slice(b_q * blk, (b_q + 1) * blk)
                diag = jnp.where(key_idx <= qry_idx, src[lanes, lanes], -1e30)
                top = jnp.max(diag, axis=0, keepdims=True)
                if b_q:
                    top = jnp.maximum(top, jnp.max(src[:b_q * blk, lanes], axis=0, keepdims=True))
                p_diag = jnp.exp2((diag - top) * scale)
                total = jnp.sum(p_diag, axis=0, keepdims=True)
                parts = [p_diag.astype(BF16)]
                if b_q:
                    p_full = jnp.exp2((src[:b_q * blk, lanes] - top) * scale)
                    total = total + jnp.sum(p_full, axis=0, keepdims=True)
                    parts.insert(0, p_full.astype(BF16))
                if b_q == t:
                    parts.append(jnp.zeros((blk, blk), BF16))
                cols.append(parts[0] if len(parts) == 1 else jnp.concatenate(parts, axis=0))
                inv.append(1.0 / total)
            probs = jnp.concatenate(cols, axis=1)
            out = jnp.dot(vc_ref[r, :, :probs.shape[0]], probs, preferred_element_type=F32)
            outs.append(out * jnp.concatenate(inv, axis=1))
        return jnp.concatenate(outs, axis=1)

    def attend(r, between, after):
        qkv[...] = nt_dot(wq[...], h_v[r]).astype(BF16)
        k_rot = rotate(qkv[q_width:q_width + head, :])
        kc_ref[r] = k_rot
        vc_ref[r] = qkv[q_width + head:, :]
        kt[...] = k_rot.astype(F32).T.astype(BF16)
        scores(0, s_a)

        def body(i, carry):
            row = pl.multiple_of(i * 2 * head, 2 * head)
            scores(row + head, s_b)
            out_a = softmax_pv(s_a, r)
            scores(jnp.minimum(row + 2 * head, q_width - head), s_a)
            out_b = softmax_pv(s_b, r)
            mixed[r, :, pl.ds(row, 2 * head)] = jnp.concatenate([out_a, out_b], axis=0).T.astype(BF16)
            return carry

        pairs = q_width // (2 * head)
        lax.fori_loop(0, pairs // 2, body, 0)
        between()
        lax.fori_loop(pairs // 2, pairs, body, 0)
        after()

    def attend_0_mid():
        pl.when(a != 2)(far_arrivals)
        start_second(0, step_b)

    def attend_1_mid():
        forward_second(0, step_b)
        start_second(0, 3)

    def attend_2_end():
        finish_second(0, step_b)
        forward_second(0, 3)

    nothing = lambda: None
    attend(0, attend_0_mid, lambda: forward_second(0, step_a))
    attend(1, attend_1_mid, nothing)
    attend(2, lambda: finish_second(0, step_a), attend_2_end)
    attend(3, last.start, lambda: finish_second(0, 3))
    last.forward()
    from_partner(0, 1)
    from_partner(0, 2)

    gate_at = q_width + 2 * head
    tok = 512
    tiles = seq // tok

    def mlp_chunk(c):
        assemble(wg, gi, in_rows, gate_at + c * chunk, chunk)
        assemble(wu, gi, in_rows, gate_at + ff + c * chunk, chunk)

        def body(i, carry):
            r = i // tiles
            rows = pl.ds(pl.multiple_of((i - r * tiles) * tok, tok), tok)
            h_t = h_v[r, rows, :]
            g = nt_dot(h_t, wg[...]).astype(BF16).astype(F32)
            u = nt_dot(h_t, wu[...]).astype(BF16).astype(F32)
            act = 0.5 * g * (1.0 + jnp.tanh(0.5 * g))
            mixed[r, rows, q_width + c * chunk:q_width + (c + 1) * chunk] = (act * u).astype(BF16)
            return carry
        lax.fori_loop(0, n_req * tiles, body, 0)

    for c in range(ff // chunk):
        mlp_chunk(c)
        if c == 0:
            from_partner(0, 3)
            last.finish()
            for s in range(n):
                start_second(1, s)
        if c == 1:
            forward_second(1, 0)
            forward_second(1, 1)
        if c == 2:
            forward_second(1, 2)
            forward_second(1, 3)
            finish_second(1, 0)
            finish_second(1, 1)
        if c == 3:
            finish_second(1, 2)
            finish_second(1, 3)
    for s in range(n):
        from_partner(1, s)

    assemble(wo, go, out_rows, 0, q_width + ff)

    def y_copy(r, t):
        rows = pl.ds(pl.multiple_of(t * tok, tok), tok)
        return pltpu.make_async_copy(x_v.at[r, rows], y_hbm.at[r, rows], y_sem.at[r, t])

    def out_body(i, carry):
        r = i // tiles
        t = i - r * tiles
        rows = pl.ds(pl.multiple_of(t * tok, tok), tok)
        acc = jnp.dot(mixed[r, rows, :], wo[...], preferred_element_type=F32)
        x_v[r, rows, :] = (x_v[r, rows, :].astype(F32) + acc).astype(BF16)
        y_copy(r, t).start()
        return carry
    lax.fori_loop(0, n_req * tiles, out_body, 0)

    for r in range(n_req):
        for t in range(tiles):
            y_copy(r, t).wait()
    for stage in range(2):
        for way in (RIGHT, LEFT):
            for p in range(parts):
                piece_copy(stage, way, p, 0).wait_send()
            for p in to_right if way == RIGHT else to_left:
                piece_copy(stage, way, p, 1).wait_send()
    last.drain()
    for rnd in range(2):
        for s in range(n):
            if rnd or s:
                second_ring(rnd, s).drain()
            for k in range(n):
                pair_copy(rnd, s, k, True).wait_send()


def rope_tables(seq, head):
    inv_freq = (np.float32(ROPE_BASE) ** (-np.arange(head // 2, dtype=np.float32) * np.float32(2.0) / np.float32(head)))
    angles = inv_freq.astype(np.float32)[:, None] * np.arange(seq, dtype=np.float32)[None, :]
    return np.cos(angles).astype(np.float32), np.sin(angles).astype(np.float32)


def solution(mesh):
    tok_spec = P(('part', 'dp', 'tp'))
    n = mesh.shape['tp']
    n_dev = n * mesh.shape['dp']

    def per_device(x_blk, ln_gain, w_in_blk, w_out_blk):
        n_req, seq, d = x_blk.shape
        in_rows, out_rows = w_in_blk.shape[1], w_out_blk.shape[0]
        ff = 4 * d
        q_width = out_rows * n_dev - ff
        head = (in_rows * n_dev - q_width - 2 * ff) // 2
        chunk = min(512, ff)
        parts = d // 128
        cos, sin = rope_tables(seq, head)
        vmem = pl.BlockSpec(memory_space=pltpu.VMEM)
        anyw = pl.BlockSpec(memory_space=pl.ANY)
        tiles = seq // 512
        y, kc, vc = pl.pallas_call(
            functools.partial(layer_kernel, n),
            out_shape=(jax.ShapeDtypeStruct(x_blk.shape, BF16),
                       jax.ShapeDtypeStruct((n_req, head, seq), BF16),
                       jax.ShapeDtypeStruct((n_req, head, seq), BF16)),
            in_specs=[anyw, vmem, anyw, anyw, vmem, vmem],
            out_specs=(anyw, vmem, vmem),
            scratch_shapes=[
                pltpu.VMEM((n_req, seq, d), BF16),
                pltpu.VMEM((n_req, seq, d), BF16),
                pltpu.VMEM((n_req, seq, q_width + ff), BF16),
                pltpu.VMEM((parts, n_dev, in_rows, d // parts), BF16),
                pltpu.VMEM((2, n_dev, out_rows, d // 2), BF16),
                pltpu.VMEM((q_width + 2 * head, d), BF16),
                pltpu.VMEM((chunk, d), BF16),
                pltpu.VMEM((chunk, d), BF16),
                pltpu.VMEM((q_width + ff, d), BF16),
                pltpu.VMEM((q_width + 2 * head, seq), BF16),
                pltpu.VMEM((seq, head), BF16),
                pltpu.VMEM((seq, seq), F32),
                pltpu.VMEM((seq, seq), F32),
                pltpu.SemaphoreType.DMA((n_req,)),
                pltpu.SemaphoreType.DMA((parts + 2,)),
                pltpu.SemaphoreType.DMA((n_req, tiles)),
                pltpu.SemaphoreType.DMA((2, 1 + n, 6)),
                pltpu.SemaphoreType.DMA((2, 1 + n, 6)),
                pltpu.SemaphoreType.DMA((2, n, n)),
                pltpu.SemaphoreType.DMA((2, n, n)),
                pltpu.SemaphoreType.DMA((2, 2, parts + parts // 2)),
                pltpu.SemaphoreType.DMA((2, 2, parts + parts // 2)),
            ],
            compiler_params=pltpu.CompilerParams(
                collective_id=0, has_side_effects=True, vmem_limit_bytes=63 * 1024 * 1024),
        )(x_blk, ln_gain, w_in_blk.T, w_out_blk, cos, sin)
        return y, kc.swapaxes(1, 2), vc.swapaxes(1, 2)

    return jax.shard_map(per_device, mesh=mesh,
                         in_specs=(tok_spec, P(), P(None, ('dp', 'tp')), P(('dp', 'tp'), None)),
                         out_specs=(tok_spec, tok_spec, tok_spec), check_vma=False)
```

```python
import functools

import jax
import jax.numpy as jnp
import numpy as np
from jax import lax
from jax.experimental import pallas as pl
from jax.experimental.pallas import tpu as pltpu
from jax.sharding import PartitionSpec as P

LN_EPS = 1e-6
ROPE_BASE = 10000.0
MESH = pl.DeviceIdType.MESH
F32 = jnp.float32
BF16 = jnp.bfloat16


def nt_dot(lhs, rhs):
    return lax.dot_general(lhs, rhs, (((1,), (1,)), ((), ())), preferred_element_type=F32)


class Ring:
    def __init__(self, n, pos, right, left, block, send, recv):
        self.n, self.pos, self.right, self.left = n, pos, right, left
        self.block, self.send, self.recv = block, send, recv
        self.routes = ((0, 0, True), (0, 1, True), (1, 0, True), (0, 1, False), (0, 0, False), (1, 1, False))

    def _copy(self, k, hops):
        back, half, to_right = self.routes[k]
        step = (back + hops) if to_right else self.n - (back + hops)
        z = lax.rem(self.pos - step + 2 * self.n, self.n)
        ref = self.block(z, half)
        return pltpu.make_async_remote_copy(
            src_ref=ref, dst_ref=ref, send_sem=self.send(k), recv_sem=self.recv(k),
            device_id=self.right if to_right else self.left, device_id_type=MESH)

    def start(self):
        for k in (0, 3, 1, 4):
            self._copy(k, 0).start()

    def forward(self):
        self._copy(0, 1).wait_recv()
        self._copy(2, 0).start()
        self._copy(3, 1).wait_recv()
        self._copy(5, 0).start()

    def finish(self):
        for k in (1, 4, 2, 5):
            self._copy(k, 1).wait_recv()

    def drain(self):
        for k in range(6):
            self._copy(k, 0).wait_send()


def layer_kernel(n, x_hbm, gain_ref, wi_hbm, wo_hbm, cos_ref, sin_ref, y_hbm, kc_ref, vc_ref,
                 x_v, h_v, mixed, gi, go, wq, wg0, wu0, wg1, wu1, wo, qkv, kt, s_a, s_b,
                 x_sem, own_sem, y_sem, send_sem, recv_sem, psend_sem, precv_sem, qsend_sem, qrecv_sem):
    n_req, seq, d = x_v.shape
    parts, _, in_rows, lanes = gi.shape
    out_rows, half = go.shape[2], go.shape[3]
    mid = parts // 2
    n_dev = gi.shape[1]
    head = kc_ref.shape[1]
    q_width = wq.shape[0] - 2 * head
    ff = wo.shape[0] - q_width
    chunk = wg0.shape[0]

    dp, tp = lax.axis_index("dp"), lax.axis_index("tp")
    core, x, y = lax.rem(dp, 2), dp // 2, tp
    a = (1 - core) * x + core * y
    b = (1 - core) * y + core * x

    def place(za, zb, c):
        zx = (1 - c) * za + c * zb
        zy = (1 - c) * zb + c * za
        return zx * 2 + c, zy

    def device(za, zb):
        zdp, ztp = place(lax.rem(za + n, n), lax.rem(zb + n, n), core)
        return {"dp": zdp, "tp": ztp}

    def shard(za, zb, c):
        zdp, ztp = place(za, zb, c)
        return zdp * n + ztp

    partner = {"dp": x * 2 + 1 - core, "tp": tp}
    bufs = (gi, go)
    me = dp * n + tp

    own = []
    for p in range(parts):
        own.append(pltpu.make_async_copy(wi_hbm.at[:, pl.ds(p * lanes, lanes)], gi.at[p, me], own_sem.at[p]))
    for h in range(2):
        own.append(pltpu.make_async_copy(wo_hbm.at[:, pl.ds(h * half, half)], go.at[h, me], own_sem.at[parts + h]))
    for copy in own:
        copy.start()
    x_in = [pltpu.make_async_copy(x_hbm.at[r], x_v.at[r], x_sem.at[r]) for r in range(n_req)]
    for copy in x_in:
        copy.start()

    barrier = pltpu.get_barrier_semaphore()
    for dev in (device(a + 1, b), device(a - 1, b), device(a, b + 1), device(a, b - 1), partner):
        pl.semaphore_signal(barrier, inc=1, device_id=dev, device_id_type=MESH)
    pl.semaphore_wait(barrier, 5)
    for copy in own:
        copy.wait()

    def piece(rnd, h, idx):
        return gi.at[pl.ds(h * mid, mid), idx] if rnd == 0 else go.at[h, idx]

    def first_ring(rnd):
        return Ring(n, a, device(a + 1, b), device(a - 1, b),
                    lambda z, h: piece(rnd, h, shard(z, b, core)),
                    lambda k: send_sem.at[rnd, 0, k], lambda k: recv_sem.at[rnd, 0, k])

    def second_ring(rnd, s):
        return Ring(n, b, device(a, b + 1), device(a, b - 1),
                    lambda z, h: piece(rnd, h, shard(s, z, core)),
                    lambda k: send_sem.at[rnd, 1 + s, k], lambda k: recv_sem.at[rnd, 1 + s, k])

    def pair_copy(rnd, s, k, mine):
        if mine:
            idx = shard(s, lax.rem(b + k, n), core)
        else:
            idx = shard(s, lax.rem(a + k, n), 1 - core)
        ref = bufs[rnd].at[:, idx]
        return pltpu.make_async_remote_copy(
            src_ref=ref, dst_ref=ref, send_sem=psend_sem.at[rnd, s, k], recv_sem=precv_sem.at[rnd, s, k],
            device_id=partner, device_id_type=MESH)

    last = first_ring(1)

    def finish_second(rnd, s):
        second_ring(rnd, s).finish()
        for k in range(1, n):
            pair_copy(rnd, s, k, True).start()

    def start_second(rnd, s):
        second_ring(rnd, s).start()
        pair_copy(rnd, s, 0, True).start()

    def from_partner(rnd, s):
        for k in range(n):
            pair_copy(rnd, s, k, False).wait_recv()

    RIGHT, LEFT = 0, 1
    to_right, to_left = range(mid), range(mid, parts)

    def piece_copy(stage, way, p, back, arriving=False):
        step = back + (1 if arriving else 0)
        pos = b if stage else a
        z = lax.rem(pos + n - step, n) if way == RIGHT else lax.rem(pos + step, n)
        ref = gi.at[p, shard(0, z, core) if stage else shard(z, b, core)]
        sem = p if back == 0 else parts + (p if way == RIGHT else p - mid)
        sign = 1 if way == RIGHT else -1
        return pltpu.make_async_remote_copy(
            src_ref=ref, dst_ref=ref, send_sem=qsend_sem.at[stage, way, sem], recv_sem=qrecv_sem.at[stage, way, sem],
            device_id=device(a, b + sign) if stage else device(a + sign, b), device_id_type=MESH)

    def send(stage, way, p, back=0):
        piece_copy(stage, way, p, back).start()

    def arrive(stage, way, p, back=0):
        piece_copy(stage, way, p, back, True).wait_recv()

    def own_all(way):
        for p in (*to_right, *to_left) if way == RIGHT else (*to_left, *to_right):
            send(0, way, p)

    def forward_all(way):
        for p in to_right if way == RIGHT else to_left:
            arrive(0, way, p)
            send(0, way, p, 1)

    def pass_on(way, p):
        arrive(1, way, p)
        send(1, way, p, 1)

    def first_step(role, i):
        mixed_order = tuple(p for pair in zip(to_right, to_left) for p in pair)
        order = {1: (*to_right, *to_left), n - 1: (*to_left, *to_right)}.get(role, mixed_order)
        p = order[i]
        if role == 1:
            arrive(0, RIGHT, p)
            if p in to_right:
                send(0, RIGHT, p, 1)
        elif role == n - 1:
            arrive(0, LEFT, p)
            if p in to_left:
                send(0, LEFT, p, 1)
        elif role:
            arrive(0, RIGHT if p in to_right else LEFT, p, 1)
        send(1, RIGHT, p)
        send(1, LEFT, p)
        if i >= mid:
            if role == 1:
                pass_on(RIGHT, i - mid)
            elif role == n - 1:
                pass_on(LEFT, i)
            elif i == mid:
                pass_on(RIGHT, 0)
                pass_on(LEFT, mid)
            elif i == parts - 1:
                for j in range(1, mid):
                    pass_on(RIGHT, j)
                    pass_on(LEFT, mid + j)

    def on_role(role, fn):
        pl.when(a == role)(fn)

    on_role(0, lambda: (own_all(RIGHT), own_all(LEFT)) and None)

    gain = gain_ref[...].reshape(1, d)
    ln_rows = 128
    per_req = seq // ln_rows

    def norm_rows(first, count):
        def body(i, carry):
            j = first + i
            r = j // per_req
            rows = pl.ds(pl.multiple_of((j - r * per_req) * ln_rows, ln_rows), ln_rows)
            xw = x_v[r, rows, :].astype(F32)
            cen = xw - jnp.mean(xw, axis=-1, keepdims=True)
            var = jnp.mean(cen * cen, axis=-1, keepdims=True)
            h_v[r, rows, :] = (cen * lax.rsqrt(var + LN_EPS) * gain).astype(BF16)
            return carry
        lax.fori_loop(0, count, body, 0)

    for copy in x_in:
        copy.wait()
    blocks = n_req * per_req
    share = blocks // (parts + 2)
    norm_rows(0, blocks - share * parts)
    for i in range(parts):
        for role in range(n):
            on_role(role, functools.partial(first_step, role, i))
        norm_rows(blocks - share * (parts - i), share)
    pair_copy(0, 0, 0, True).start()
    pl.when(a != 0)(lambda: (own_all(RIGHT), own_all(LEFT)) and None)
    on_role(1, lambda: [pass_on(LEFT, p) for p in to_left] and None)
    on_role(n - 1, lambda: [pass_on(RIGHT, p) for p in to_right] and None)
    for p in to_left:
        arrive(1, RIGHT, p)
    pair_copy(0, 0, n - 1, True).start()
    for p in to_right:
        arrive(1, LEFT, p)
    pair_copy(0, 0, 1, True).start()
    for p in to_right:
        arrive(1, RIGHT, p, 1)
    for p in to_left:
        arrive(1, LEFT, p, 1)
    pair_copy(0, 0, 2, True).start()

    pl.when(a != 1)(lambda: forward_all(RIGHT))
    pl.when(a != n - 1)(lambda: forward_all(LEFT))

    @pl.when(a != 1)
    def _():
        for p in to_left:
            arrive(0, RIGHT, p)

    @pl.when(a != n - 1)
    def _():
        for p in to_right:
            arrive(0, LEFT, p)

    def far_arrivals():
        for p in to_right:
            arrive(0, RIGHT, p, 1)
        for p in to_left:
            arrive(0, LEFT, p, 1)

    def forward_second(rnd, s):
        second_ring(rnd, s).forward()

    step_a = 1 + a // (n - 1)
    step_b = 3 - step_a
    start_second(0, step_a)
    from_partner(0, 0)

    def assemble(dst, src, rows_per, start, count):
        row = start
        while row < start + count:
            blk, r0 = row // rows_per, row % rows_per
            take = min(rows_per - r0, start + count - row)
            width = src.shape[3]
            for h in range(src.shape[0]):
                dst[row - start:row - start + take, h * width:(h + 1) * width] = src[h, blk, r0:r0 + take, :]
            row += take

    assemble(wq, gi, in_rows, 0, q_width + 2 * head)

    hd2 = head // 2
    scale = float(head ** -0.5 * np.log2(np.e))
    blk = 128
    n_blk = seq // blk
    key_idx = lax.broadcasted_iota(jnp.int32, (blk, blk), 0)
    qry_idx = lax.broadcasted_iota(jnp.int32, (blk, blk), 1)

    def rotate(u):
        cos, sin = cos_ref[...], sin_ref[...]
        first, second = u[:hd2].astype(F32), u[hd2:].astype(F32)
        return jnp.concatenate([first * cos - second * sin, second * cos + first * sin], axis=0).astype(BF16)

    def scores(row, dst):
        q_rot = rotate(qkv[pl.ds(row, head), :])
        for t in range(0, seq, 2 * blk):
            stop = t + 2 * blk
            dst[:stop, t:stop] = jnp.dot(kt[:stop], q_rot[:, t:stop], preferred_element_type=F32)

    def softmax_pv(src, r):
        outs = []
        for t in range(0, n_blk, 2):
            cols, inv = [], []
            for b_q in (t, t + 1):
                lanes = slice(b_q * blk, (b_q + 1) * blk)
                diag = jnp.where(key_idx <= qry_idx, src[lanes, lanes], -1e30)
                top = jnp.max(diag, axis=0, keepdims=True)
                if b_q:
                    top = jnp.maximum(top, jnp.max(src[:b_q * blk, lanes], axis=0, keepdims=True))
                p_diag = jnp.exp2((diag - top) * scale)
                total = jnp.sum(p_diag, axis=0, keepdims=True)
                parts = [p_diag.astype(BF16)]
                if b_q:
                    p_full = jnp.exp2((src[:b_q * blk, lanes] - top) * scale)
                    total = total + jnp.sum(p_full, axis=0, keepdims=True)
                    parts.insert(0, p_full.astype(BF16))
                if b_q == t:
                    parts.append(jnp.zeros((blk, blk), BF16))
                cols.append(parts[0] if len(parts) == 1 else jnp.concatenate(parts, axis=0))
                inv.append(1.0 / total)
            probs = jnp.concatenate(cols, axis=1)
            out = jnp.dot(vc_ref[r, :, :probs.shape[0]], probs, preferred_element_type=F32)
            outs.append(out * jnp.concatenate(inv, axis=1))
        return jnp.concatenate(outs, axis=1)

    def attend(r, between, after):
        qkv[...] = nt_dot(wq[...], h_v[r]).astype(BF16)
        k_rot = rotate(qkv[q_width:q_width + head, :])
        kc_ref[r] = k_rot
        vc_ref[r] = qkv[q_width + head:, :]
        kt[...] = k_rot.astype(F32).T.astype(BF16)
        scores(0, s_a)

        def body(i, carry):
            row = pl.multiple_of(i * 2 * head, 2 * head)
            scores(row + head, s_b)
            out_a = softmax_pv(s_a, r)
            scores(jnp.minimum(row + 2 * head, q_width - head), s_a)
            out_b = softmax_pv(s_b, r)
            mixed[r, :, pl.ds(row, 2 * head)] = jnp.concatenate([out_a, out_b], axis=0).T.astype(BF16)
            return carry

        pairs = q_width // (2 * head)
        lax.fori_loop(0, pairs // 2, body, 0)
        between()
        lax.fori_loop(pairs // 2, pairs, body, 0)
        after()

    def attend_0_mid():
        pl.when(a != 2)(far_arrivals)
        start_second(0, step_b)

    def attend_1_mid():
        forward_second(0, step_b)
        start_second(0, 3)

    def attend_2_end():
        finish_second(0, step_b)
        forward_second(0, 3)

    mids = (attend_0_mid, attend_1_mid, lambda: finish_second(0, step_a), last.start)
    ends = (lambda: forward_second(0, step_a), None, attend_2_end, lambda: finish_second(0, 3))

    def steps(r, todo):
        for at, fn in enumerate(todo):
            if fn is not None:
                pl.when(r == at)(fn)

    def request(r, carry):
        attend(r, lambda: steps(r, mids), lambda: steps(r, ends))
        return carry

    lax.fori_loop(0, n_req, request, 0)
    last.forward()
    from_partner(0, 1)
    from_partner(0, 2)

    gate_at = q_width + 2 * head
    tok = 512
    tiles = seq // tok

    tokens = n_req * seq
    columns = ((wg0, wu0), (wg1, wu1))
    n_chunks = ff // chunk

    def gather_chunk(c):
        wg, wu = columns[c % 2]
        assemble(wg, gi, in_rows, gate_at + c * chunk, chunk)
        assemble(wu, gi, in_rows, gate_at + ff + c * chunk, chunk)

    def mlp_chunk(c):
        wg, wu = columns[c % 2]
        h_t = h_v[...].reshape(tokens, d)
        g = nt_dot(h_t, wg[...]).astype(BF16).astype(F32)
        u = nt_dot(h_t, wu[...]).astype(BF16).astype(F32)
        act = 0.5 * g * (1.0 + jnp.tanh(0.5 * g))
        mixed[:, :, q_width + c * chunk:q_width + (c + 1) * chunk] = (act * u).astype(BF16).reshape(n_req, seq, chunk)

    gather_chunk(0)
    for c in range(n_chunks):
        if c == 1:
            from_partner(0, 3)
        if c + 1 < n_chunks and c:
            gather_chunk(c + 1)
        mlp_chunk(c)
        if c == 0:
            gather_chunk(1)
        if c == 1:
            last.finish()
            for s in range(n):
                start_second(1, s)
        if c == 4:
            forward_second(1, 0)
            forward_second(1, 1)
        if c == 6:
            forward_second(1, 2)
            forward_second(1, 3)
            finish_second(1, 0)
            finish_second(1, 1)
        if c == 8:
            finish_second(1, 2)
            finish_second(1, 3)
    for s in range(n):
        from_partner(1, s)

    assemble(wo, go, out_rows, 0, q_width + ff)

    def y_copy(r, t):
        rows = pl.ds(pl.multiple_of(t * tok, tok), tok)
        return pltpu.make_async_copy(x_v.at[r, rows], y_hbm.at[r, rows], y_sem.at[r, t])

    def out_body(i, carry):
        r = i // tiles
        t = i - r * tiles
        rows = pl.ds(pl.multiple_of(t * tok, tok), tok)
        acc = jnp.dot(mixed[r, rows, :], wo[...], preferred_element_type=F32)
        x_v[r, rows, :] = (x_v[r, rows, :].astype(F32) + acc).astype(BF16)
        y_copy(r, t).start()
        return carry
    lax.fori_loop(0, n_req * tiles, out_body, 0)

    for r in range(n_req):
        for t in range(tiles):
            y_copy(r, t).wait()
    for stage in range(2):
        for way in (RIGHT, LEFT):
            for p in range(parts):
                piece_copy(stage, way, p, 0).wait_send()
            for p in to_right if way == RIGHT else to_left:
                piece_copy(stage, way, p, 1).wait_send()
    last.drain()
    for rnd in range(2):
        for s in range(n):
            if rnd or s:
                second_ring(rnd, s).drain()
            for k in range(n):
                pair_copy(rnd, s, k, True).wait_send()


def rope_tables(seq, head):
    inv_freq = (np.float32(ROPE_BASE) ** (-np.arange(head // 2, dtype=np.float32) * np.float32(2.0) / np.float32(head)))
    angles = inv_freq.astype(np.float32)[:, None] * np.arange(seq, dtype=np.float32)[None, :]
    return np.cos(angles).astype(np.float32), np.sin(angles).astype(np.float32)


def solution(mesh):
    tok_spec = P(('part', 'dp', 'tp'))
    n = mesh.shape['tp']
    n_dev = n * mesh.shape['dp']

    def per_device(x_blk, ln_gain, w_in_blk, w_out_blk):
        n_req, seq, d = x_blk.shape
        in_rows, out_rows = w_in_blk.shape[1], w_out_blk.shape[0]
        ff = 4 * d
        q_width = out_rows * n_dev - ff
        head = (in_rows * n_dev - q_width - 2 * ff) // 2
        chunk = 256
        parts = d // 128
        cos, sin = rope_tables(seq, head)
        vmem = pl.BlockSpec(memory_space=pltpu.VMEM)
        anyw = pl.BlockSpec(memory_space=pl.ANY)
        tiles = seq // 512
        y, kc, vc = pl.pallas_call(
            functools.partial(layer_kernel, n),
            out_shape=(jax.ShapeDtypeStruct(x_blk.shape, BF16),
                       jax.ShapeDtypeStruct((n_req, head, seq), BF16),
                       jax.ShapeDtypeStruct((n_req, head, seq), BF16)),
            in_specs=[anyw, vmem, anyw, anyw, vmem, vmem],
            out_specs=(anyw, vmem, vmem),
            scratch_shapes=[
                pltpu.VMEM((n_req, seq, d), BF16),
                pltpu.VMEM((n_req, seq, d), BF16),
                pltpu.VMEM((n_req, seq, q_width + ff), BF16),
                pltpu.VMEM((parts, n_dev, in_rows, d // parts), BF16),
                pltpu.VMEM((2, n_dev, out_rows, d // 2), BF16),
                pltpu.VMEM((q_width + 2 * head, d), BF16),
                pltpu.VMEM((chunk, d), BF16),
                pltpu.VMEM((chunk, d), BF16),
                pltpu.VMEM((chunk, d), BF16),
                pltpu.VMEM((chunk, d), BF16),
                pltpu.VMEM((q_width + ff, d), BF16),
                pltpu.VMEM((q_width + 2 * head, seq), BF16),
                pltpu.VMEM((seq, head), BF16),
                pltpu.VMEM((seq, seq), F32),
                pltpu.VMEM((seq, seq), F32),
                pltpu.SemaphoreType.DMA((n_req,)),
                pltpu.SemaphoreType.DMA((parts + 2,)),
                pltpu.SemaphoreType.DMA((n_req, tiles)),
                pltpu.SemaphoreType.DMA((2, 1 + n, 6)),
                pltpu.SemaphoreType.DMA((2, 1 + n, 6)),
                pltpu.SemaphoreType.DMA((2, n, n)),
                pltpu.SemaphoreType.DMA((2, n, n)),
                pltpu.SemaphoreType.DMA((2, 2, parts + parts // 2)),
                pltpu.SemaphoreType.DMA((2, 2, parts + parts // 2)),
            ],
            compiler_params=pltpu.CompilerParams(
                collective_id=0, has_side_effects=True,
                vmem_limit_bytes=63 * 1024 * 1024),
        )(x_blk, ln_gain, w_in_blk.T, w_out_blk, cos, sin)
        return y, kc.swapaxes(1, 2), vc.swapaxes(1, 2)

    return jax.shard_map(per_device, mesh=mesh,
                         in_specs=(tok_spec, P(), P(None, ('dp', 'tp')), P(('dp', 'tp'), None)),
                         out_specs=(tok_spec, tok_spec, tok_spec), check_vma=False)
```

```python
import functools

import jax
import jax.numpy as jnp
import numpy as np
from jax import lax
from jax.experimental import pallas as pl
from jax.experimental.pallas import tpu as pltpu
from jax.sharding import PartitionSpec as P

LN_EPS = 1e-6
ROPE_BASE = 10000.0
MESH = pl.DeviceIdType.MESH
F32 = jnp.float32
BF16 = jnp.bfloat16


def nt_dot(lhs, rhs):
    return lax.dot_general(lhs, rhs, (((1,), (1,)), ((), ())), preferred_element_type=F32)


class Ring:
    def __init__(self, n, pos, right, left, block, send, recv):
        self.n, self.pos, self.right, self.left = n, pos, right, left
        self.block, self.send, self.recv = block, send, recv
        self.routes = ((0, 0, True), (0, 1, True), (1, 0, True), (0, 1, False), (0, 0, False), (1, 1, False))

    def _copy(self, k, hops):
        back, half, to_right = self.routes[k]
        step = (back + hops) if to_right else self.n - (back + hops)
        z = lax.rem(self.pos - step + 2 * self.n, self.n)
        ref = self.block(z, half)
        return pltpu.make_async_remote_copy(
            src_ref=ref, dst_ref=ref, send_sem=self.send(k), recv_sem=self.recv(k),
            device_id=self.right if to_right else self.left, device_id_type=MESH)

    def start(self):
        for k in (0, 3, 1, 4):
            self._copy(k, 0).start()

    def forward(self):
        self._copy(0, 1).wait_recv()
        self._copy(2, 0).start()
        self._copy(3, 1).wait_recv()
        self._copy(5, 0).start()

    def finish(self):
        for k in (1, 4, 2, 5):
            self._copy(k, 1).wait_recv()

    def drain(self):
        for k in range(6):
            self._copy(k, 0).wait_send()


def layer_kernel(n, x_hbm, gain_ref, wi_hbm, wo_hbm, cos_ref, sin_ref, y_hbm, kc_ref, vc_ref,
                 x_v, h_v, mixed, gi, go, wq, wg0, wu0, wg1, wu1, wo, qkv, kt, s_a, s_b,
                 x_sem, own_sem, y_sem, send_sem, recv_sem, psend_sem, precv_sem, qsend_sem, qrecv_sem):
    n_req, seq, d = x_v.shape
    parts, _, in_rows, lanes = gi.shape
    out_rows, half = go.shape[2], go.shape[3]
    mid = parts // 2
    n_dev = gi.shape[1]
    head = kc_ref.shape[1]
    q_width = wq.shape[0] - 2 * head
    ff = wo.shape[0] - q_width
    chunk = wg0.shape[0]

    dp, tp = lax.axis_index("dp"), lax.axis_index("tp")
    core, x, y = lax.rem(dp, 2), dp // 2, tp
    a = (1 - core) * x + core * y
    b = (1 - core) * y + core * x

    def place(za, zb, c):
        zx = (1 - c) * za + c * zb
        zy = (1 - c) * zb + c * za
        return zx * 2 + c, zy

    def device(za, zb):
        zdp, ztp = place(lax.rem(za + n, n), lax.rem(zb + n, n), core)
        return {"dp": zdp, "tp": ztp}

    def shard(za, zb, c):
        zdp, ztp = place(za, zb, c)
        return zdp * n + ztp

    partner = {"dp": x * 2 + 1 - core, "tp": tp}
    bufs = (gi, go)
    me = dp * n + tp

    own = []
    for p in range(parts):
        own.append(pltpu.make_async_copy(wi_hbm.at[:, pl.ds(p * lanes, lanes)], gi.at[p, me], own_sem.at[p]))
    for h in range(2):
        own.append(pltpu.make_async_copy(wo_hbm.at[:, pl.ds(h * half, half)], go.at[h, me], own_sem.at[parts + h]))
    for copy in own:
        copy.start()
    x_in = [pltpu.make_async_copy(x_hbm.at[r], x_v.at[r], x_sem.at[r]) for r in range(n_req)]
    for copy in x_in:
        copy.start()

    barrier = pltpu.get_barrier_semaphore()
    for dev in (device(a + 1, b), device(a - 1, b), device(a, b + 1), device(a, b - 1), partner):
        pl.semaphore_signal(barrier, inc=1, device_id=dev, device_id_type=MESH)
    pl.semaphore_wait(barrier, 5)
    for copy in own:
        copy.wait()

    def piece(rnd, h, idx):
        return gi.at[pl.ds(h * mid, mid), idx] if rnd == 0 else go.at[h, idx]

    def first_ring(rnd):
        return Ring(n, a, device(a + 1, b), device(a - 1, b),
                    lambda z, h: piece(rnd, h, shard(z, b, core)),
                    lambda k: send_sem.at[rnd, 0, k], lambda k: recv_sem.at[rnd, 0, k])

    def second_ring(rnd, s):
        return Ring(n, b, device(a, b + 1), device(a, b - 1),
                    lambda z, h: piece(rnd, h, shard(s, z, core)),
                    lambda k: send_sem.at[rnd, 1 + s, k], lambda k: recv_sem.at[rnd, 1 + s, k])

    def pair_copy(rnd, s, k, mine):
        if mine:
            idx = shard(s, lax.rem(b + k, n), core)
        else:
            idx = shard(s, lax.rem(a + k, n), 1 - core)
        ref = bufs[rnd].at[:, idx]
        return pltpu.make_async_remote_copy(
            src_ref=ref, dst_ref=ref, send_sem=psend_sem.at[rnd, s, k], recv_sem=precv_sem.at[rnd, s, k],
            device_id=partner, device_id_type=MESH)

    last = first_ring(1)

    def finish_second(rnd, s):
        second_ring(rnd, s).finish()
        for k in range(1, n):
            pair_copy(rnd, s, k, True).start()

    def start_second(rnd, s):
        second_ring(rnd, s).start()
        pair_copy(rnd, s, 0, True).start()

    def from_partner(rnd, s):
        for k in range(n):
            pair_copy(rnd, s, k, False).wait_recv()

    RIGHT, LEFT = 0, 1
    to_right, to_left = range(mid), range(mid, parts)

    def piece_copy(stage, way, p, back, arriving=False):
        step = back + (1 if arriving else 0)
        pos = b if stage else a
        z = lax.rem(pos + n - step, n) if way == RIGHT else lax.rem(pos + step, n)
        ref = gi.at[p, shard(0, z, core) if stage else shard(z, b, core)]
        sem = p if back == 0 else parts + (p if way == RIGHT else p - mid)
        sign = 1 if way == RIGHT else -1
        return pltpu.make_async_remote_copy(
            src_ref=ref, dst_ref=ref, send_sem=qsend_sem.at[stage, way, sem], recv_sem=qrecv_sem.at[stage, way, sem],
            device_id=device(a, b + sign) if stage else device(a + sign, b), device_id_type=MESH)

    def send(stage, way, p, back=0):
        piece_copy(stage, way, p, back).start()

    def arrive(stage, way, p, back=0):
        piece_copy(stage, way, p, back, True).wait_recv()

    def own_all(way):
        for p in (*to_right, *to_left) if way == RIGHT else (*to_left, *to_right):
            send(0, way, p)

    def forward_all(way):
        for p in to_right if way == RIGHT else to_left:
            arrive(0, way, p)
            send(0, way, p, 1)

    def pass_on(way, p):
        arrive(1, way, p)
        send(1, way, p, 1)

    def first_step(role, i):
        mixed_order = tuple(p for pair in zip(to_right, to_left) for p in pair)
        order = {1: (*to_right, *to_left), n - 1: (*to_left, *to_right)}.get(role, mixed_order)
        p = order[i]
        if role == 1:
            arrive(0, RIGHT, p)
            if p in to_right:
                send(0, RIGHT, p, 1)
        elif role == n - 1:
            arrive(0, LEFT, p)
            if p in to_left:
                send(0, LEFT, p, 1)
        elif role:
            arrive(0, RIGHT if p in to_right else LEFT, p, 1)
        send(1, RIGHT, p)
        send(1, LEFT, p)
        if role == 1 and i == mid - 1:
            own_all(RIGHT)
        if role == n - 1 and i == mid - 1:
            own_all(LEFT)
        if i >= mid:
            if role == 1:
                pass_on(RIGHT, i - mid)
            elif role == n - 1:
                pass_on(LEFT, i)
            elif i == mid:
                pass_on(RIGHT, 0)
                pass_on(LEFT, mid)
            elif i == parts - 1:
                for j in range(1, mid):
                    pass_on(RIGHT, j)
                    pass_on(LEFT, mid + j)

    def on_role(role, fn):
        pl.when(a == role)(fn)

    on_role(0, lambda: (own_all(RIGHT), own_all(LEFT)) and None)
    on_role(1, lambda: own_all(LEFT))
    on_role(n - 1, lambda: own_all(RIGHT))
    on_role(2, lambda: (own_all(RIGHT), own_all(LEFT)) and None)

    gain = gain_ref[...].reshape(1, d)
    ln_rows = 128
    per_req = seq // ln_rows

    def norm_rows(first, count):
        def body(i, carry):
            j = first + i
            r = j // per_req
            rows = pl.ds(pl.multiple_of((j - r * per_req) * ln_rows, ln_rows), ln_rows)
            xw = x_v[r, rows, :].astype(F32)
            cen = xw - jnp.mean(xw, axis=-1, keepdims=True)
            var = jnp.mean(cen * cen, axis=-1, keepdims=True)
            h_v[r, rows, :] = (cen * lax.rsqrt(var + LN_EPS) * gain).astype(BF16)
            return carry
        lax.fori_loop(0, count, body, 0)

    for copy in x_in:
        copy.wait()
    blocks = n_req * per_req
    share = blocks // (parts + 2)
    norm_rows(0, blocks - share * parts)
    for i in range(parts):
        for role in range(n):
            on_role(role, functools.partial(first_step, role, i))
        norm_rows(blocks - share * (parts - i), share)
    pair_copy(0, 0, 0, True).start()
    on_role(1, lambda: [pass_on(LEFT, p) for p in to_left] and None)
    on_role(n - 1, lambda: [pass_on(RIGHT, p) for p in to_right] and None)
    for p in to_left:
        arrive(1, RIGHT, p)
    pair_copy(0, 0, n - 1, True).start()
    for p in to_right:
        arrive(1, LEFT, p)
    pair_copy(0, 0, 1, True).start()
    for p in to_right:
        arrive(1, RIGHT, p, 1)
    for p in to_left:
        arrive(1, LEFT, p, 1)
    pair_copy(0, 0, 2, True).start()

    pl.when(a != 1)(lambda: forward_all(RIGHT))
    pl.when(a != n - 1)(lambda: forward_all(LEFT))

    @pl.when(a != 1)
    def _():
        for p in to_left:
            arrive(0, RIGHT, p)

    @pl.when(a != n - 1)
    def _():
        for p in to_right:
            arrive(0, LEFT, p)

    def far_arrivals():
        for p in to_right:
            arrive(0, RIGHT, p, 1)
        for p in to_left:
            arrive(0, LEFT, p, 1)

    def forward_second(rnd, s):
        second_ring(rnd, s).forward()

    step_a = 1 + a // (n - 1)
    step_b = 3 - step_a
    start_second(0, step_a)
    from_partner(0, 0)

    def assemble(dst, src, rows_per, start, count):
        row = start
        while row < start + count:
            blk, r0 = row // rows_per, row % rows_per
            take = min(rows_per - r0, start + count - row)
            width = src.shape[3]
            for h in range(src.shape[0]):
                dst[row - start:row - start + take, h * width:(h + 1) * width] = src[h, blk, r0:r0 + take, :]
            row += take

    assemble(wq, gi, in_rows, 0, q_width + 2 * head)

    hd2 = head // 2
    scale = float(head ** -0.5 * np.log2(np.e))
    blk = 128
    n_blk = seq // blk
    key_idx = lax.broadcasted_iota(jnp.int32, (blk, blk), 0)
    qry_idx = lax.broadcasted_iota(jnp.int32, (blk, blk), 1)

    def rotate(u):
        cos, sin = cos_ref[...], sin_ref[...]
        first, second = u[:hd2].astype(F32), u[hd2:].astype(F32)
        return jnp.concatenate([first * cos - second * sin, second * cos + first * sin], axis=0).astype(BF16)

    def scores(row, dst):
        q_rot = rotate(qkv[pl.ds(row, head), :])
        for t in range(0, seq, 2 * blk):
            stop = t + 2 * blk
            dst[:stop, t:stop] = jnp.dot(kt[:stop], q_rot[:, t:stop], preferred_element_type=F32)

    def softmax_pv(src, r):
        outs = []
        for t in range(0, n_blk, 2):
            cols, inv = [], []
            for b_q in (t, t + 1):
                lanes = slice(b_q * blk, (b_q + 1) * blk)
                diag = jnp.where(key_idx <= qry_idx, src[lanes, lanes], -1e30)
                top = jnp.max(diag, axis=0, keepdims=True)
                if b_q:
                    top = jnp.maximum(top, jnp.max(src[:b_q * blk, lanes], axis=0, keepdims=True))
                p_diag = jnp.exp2((diag - top) * scale)
                total = jnp.sum(p_diag, axis=0, keepdims=True)
                parts = [p_diag.astype(BF16)]
                if b_q:
                    p_full = jnp.exp2((src[:b_q * blk, lanes] - top) * scale)
                    total = total + jnp.sum(p_full, axis=0, keepdims=True)
                    parts.insert(0, p_full.astype(BF16))
                if b_q == t:
                    parts.append(jnp.zeros((blk, blk), BF16))
                cols.append(parts[0] if len(parts) == 1 else jnp.concatenate(parts, axis=0))
                inv.append(1.0 / total)
            probs = jnp.concatenate(cols, axis=1)
            out = jnp.dot(vc_ref[r, :, :probs.shape[0]], probs, preferred_element_type=F32)
            outs.append(out * jnp.concatenate(inv, axis=1))
        return jnp.concatenate(outs, axis=1)

    def attend(r, between, after):
        qkv[...] = nt_dot(wq[...], h_v[r]).astype(BF16)
        k_rot = rotate(qkv[q_width:q_width + head, :])
        kc_ref[r] = k_rot
        vc_ref[r] = qkv[q_width + head:, :]
        kt[...] = k_rot.astype(F32).T.astype(BF16)
        scores(0, s_a)

        def body(i, carry):
            row = pl.multiple_of(i * 2 * head, 2 * head)
            scores(row + head, s_b)
            out_a = softmax_pv(s_a, r)
            scores(jnp.minimum(row + 2 * head, q_width - head), s_a)
            out_b = softmax_pv(s_b, r)
            mixed[r, :, pl.ds(row, 2 * head)] = jnp.concatenate([out_a, out_b], axis=0).T.astype(BF16)
            return carry

        pairs = q_width // (2 * head)
        lax.fori_loop(0, pairs // 2, body, 0)
        between()
        lax.fori_loop(pairs // 2, pairs, body, 0)
        after()

    def attend_0_mid():
        pl.when(a != 2)(far_arrivals)
        start_second(0, step_b)

    def attend_1_mid():
        forward_second(0, step_b)
        start_second(0, 3)

    def attend_2_end():
        finish_second(0, step_b)
        forward_second(0, 3)

    mids = (attend_0_mid, attend_1_mid, lambda: finish_second(0, step_a), last.start)
    ends = (lambda: forward_second(0, step_a), None, attend_2_end, lambda: finish_second(0, 3))

    def steps(r, todo):
        for at, fn in enumerate(todo):
            if fn is not None:
                pl.when(r == at)(fn)

    def request(r, carry):
        attend(r, lambda: steps(r, mids), lambda: steps(r, ends))
        return carry

    lax.fori_loop(0, n_req, request, 0)
    last.forward()
    from_partner(0, 1)
    from_partner(0, 2)

    gate_at = q_width + 2 * head
    tok = 512
    tiles = seq // tok

    tokens = n_req * seq
    columns = ((wg0, wu0), (wg1, wu1))
    n_chunks = ff // chunk

    def gather_chunk(c):
        wg, wu = columns[c % 2]
        assemble(wg, gi, in_rows, gate_at + c * chunk, chunk)
        assemble(wu, gi, in_rows, gate_at + ff + c * chunk, chunk)

    def mlp_chunk(c):
        wg, wu = columns[c % 2]
        h_t = h_v[...].reshape(tokens, d)
        g = nt_dot(h_t, wg[...]).astype(BF16).astype(F32)
        u = nt_dot(h_t, wu[...]).astype(BF16).astype(F32)
        act = 0.5 * g * (1.0 + jnp.tanh(0.5 * g))
        mixed[:, :, q_width + c * chunk:q_width + (c + 1) * chunk] = (act * u).astype(BF16).reshape(n_req, seq, chunk)

    gather_chunk(0)
    for c in range(n_chunks):
        if c == 1:
            from_partner(0, 3)
        if c + 1 < n_chunks and c:
            gather_chunk(c + 1)
        mlp_chunk(c)
        if c == 0:
            gather_chunk(1)
        if c == 1:
            last.finish()
            for s in range(n):
                start_second(1, s)
        if c == 4:
            forward_second(1, 0)
            forward_second(1, 1)
        if c == 6:
            forward_second(1, 2)
            forward_second(1, 3)
            finish_second(1, 0)
            finish_second(1, 1)
        if c == 8:
            finish_second(1, 2)
            finish_second(1, 3)
    for s in range(n):
        from_partner(1, s)

    assemble(wo, go, out_rows, 0, q_width + ff)

    def y_copy(r, t):
        rows = pl.ds(pl.multiple_of(t * tok, tok), tok)
        return pltpu.make_async_copy(x_v.at[r, rows], y_hbm.at[r, rows], y_sem.at[r, t])

    def out_body(i, carry):
        r = i // tiles
        t = i - r * tiles
        rows = pl.ds(pl.multiple_of(t * tok, tok), tok)
        acc = jnp.dot(mixed[r, rows, :], wo[...], preferred_element_type=F32)
        x_v[r, rows, :] = (x_v[r, rows, :].astype(F32) + acc).astype(BF16)
        y_copy(r, t).start()
        return carry
    lax.fori_loop(0, n_req * tiles, out_body, 0)

    for r in range(n_req):
        for t in range(tiles):
            y_copy(r, t).wait()
    for stage in range(2):
        for way in (RIGHT, LEFT):
            for p in range(parts):
                piece_copy(stage, way, p, 0).wait_send()
            for p in to_right if way == RIGHT else to_left:
                piece_copy(stage, way, p, 1).wait_send()
    last.drain()
    for rnd in range(2):
        for s in range(n):
            if rnd or s:
                second_ring(rnd, s).drain()
            for k in range(n):
                pair_copy(rnd, s, k, True).wait_send()


def rope_tables(seq, head):
    inv_freq = (np.float32(ROPE_BASE) ** (-np.arange(head // 2, dtype=np.float32) * np.float32(2.0) / np.float32(head)))
    angles = inv_freq.astype(np.float32)[:, None] * np.arange(seq, dtype=np.float32)[None, :]
    return np.cos(angles).astype(np.float32), np.sin(angles).astype(np.float32)


def solution(mesh):
    tok_spec = P(('part', 'dp', 'tp'))
    n = mesh.shape['tp']
    n_dev = n * mesh.shape['dp']

    def per_device(x_blk, ln_gain, w_in_blk, w_out_blk):
        n_req, seq, d = x_blk.shape
        in_rows, out_rows = w_in_blk.shape[1], w_out_blk.shape[0]
        ff = 4 * d
        q_width = out_rows * n_dev - ff
        head = (in_rows * n_dev - q_width - 2 * ff) // 2
        chunk = 256
        parts = d // 128
        cos, sin = rope_tables(seq, head)
        vmem = pl.BlockSpec(memory_space=pltpu.VMEM)
        anyw = pl.BlockSpec(memory_space=pl.ANY)
        tiles = seq // 512
        y, kc, vc = pl.pallas_call(
            functools.partial(layer_kernel, n),
            out_shape=(jax.ShapeDtypeStruct(x_blk.shape, BF16),
                       jax.ShapeDtypeStruct((n_req, head, seq), BF16),
                       jax.ShapeDtypeStruct((n_req, head, seq), BF16)),
            in_specs=[anyw, vmem, anyw, anyw, vmem, vmem],
            out_specs=(anyw, vmem, vmem),
            scratch_shapes=[
                pltpu.VMEM((n_req, seq, d), BF16),
                pltpu.VMEM((n_req, seq, d), BF16),
                pltpu.VMEM((n_req, seq, q_width + ff), BF16),
                pltpu.VMEM((parts, n_dev, in_rows, d // parts), BF16),
                pltpu.VMEM((2, n_dev, out_rows, d // 2), BF16),
                pltpu.VMEM((q_width + 2 * head, d), BF16),
                pltpu.VMEM((chunk, d), BF16),
                pltpu.VMEM((chunk, d), BF16),
                pltpu.VMEM((chunk, d), BF16),
                pltpu.VMEM((chunk, d), BF16),
                pltpu.VMEM((q_width + ff, d), BF16),
                pltpu.VMEM((q_width + 2 * head, seq), BF16),
                pltpu.VMEM((seq, head), BF16),
                pltpu.VMEM((seq, seq), F32),
                pltpu.VMEM((seq, seq), F32),
                pltpu.SemaphoreType.DMA((n_req,)),
                pltpu.SemaphoreType.DMA((parts + 2,)),
                pltpu.SemaphoreType.DMA((n_req, tiles)),
                pltpu.SemaphoreType.DMA((2, 1 + n, 6)),
                pltpu.SemaphoreType.DMA((2, 1 + n, 6)),
                pltpu.SemaphoreType.DMA((2, n, n)),
                pltpu.SemaphoreType.DMA((2, n, n)),
                pltpu.SemaphoreType.DMA((2, 2, parts + parts // 2)),
                pltpu.SemaphoreType.DMA((2, 2, parts + parts // 2)),
            ],
            compiler_params=pltpu.CompilerParams(
                collective_id=0, has_side_effects=True,
                vmem_limit_bytes=63 * 1024 * 1024),
        )(x_blk, ln_gain, w_in_blk.T, w_out_blk, cos, sin)
        return y, kc.swapaxes(1, 2), vc.swapaxes(1, 2)

    return jax.shard_map(per_device, mesh=mesh,
                         in_specs=(tok_spec, P(), P(None, ('dp', 'tp')), P(('dp', 'tp'), None)),
                         out_specs=(tok_spec, tok_spec, tok_spec), check_vma=False)
```

```python
import functools

import jax
import jax.numpy as jnp
import numpy as np
from jax import lax
from jax.experimental import pallas as pl
from jax.experimental.pallas import tpu as pltpu
from jax.sharding import PartitionSpec as P

LN_EPS = 1e-6
ROPE_BASE = 10000.0
MESH = pl.DeviceIdType.MESH
F32 = jnp.float32
BF16 = jnp.bfloat16


def nt_dot(lhs, rhs):
    return lax.dot_general(lhs, rhs, (((1,), (1,)), ((), ())), preferred_element_type=F32)


class Ring:
    def __init__(self, n, pos, right, left, block, send, recv):
        self.n, self.pos, self.right, self.left = n, pos, right, left
        self.block, self.send, self.recv = block, send, recv
        self.routes = ((0, 0, True), (0, 1, True), (1, 0, True), (0, 1, False), (0, 0, False), (1, 1, False))

    def _copy(self, k, hops):
        back, half, to_right = self.routes[k]
        step = (back + hops) if to_right else self.n - (back + hops)
        z = lax.rem(self.pos - step + 2 * self.n, self.n)
        ref = self.block(z, half)
        return pltpu.make_async_remote_copy(
            src_ref=ref, dst_ref=ref, send_sem=self.send(k), recv_sem=self.recv(k),
            device_id=self.right if to_right else self.left, device_id_type=MESH)

    def start(self):
        for k in (0, 3, 1, 4):
            self._copy(k, 0).start()

    def forward(self):
        self._copy(0, 1).wait_recv()
        self._copy(2, 0).start()
        self._copy(3, 1).wait_recv()
        self._copy(5, 0).start()

    def finish(self):
        for k in (1, 4, 2, 5):
            self._copy(k, 1).wait_recv()

    def drain(self):
        for k in range(6):
            self._copy(k, 0).wait_send()


def layer_kernel(n, x_hbm, gain_ref, wi_hbm, wo_hbm, cos_ref, sin_ref, y_hbm, kc_ref, vc_ref,
                 x_v, h_v, mixed, gi, go, wq, wg0, wu0, wg1, wu1, wo, qkv, kt, s_a, s_b,
                 x_sem, own_sem, y_sem, send_sem, recv_sem, psend_sem, precv_sem, qsend_sem, qrecv_sem):
    n_req, seq, d = x_v.shape
    parts, _, in_rows, lanes = gi.shape
    out_rows, half = go.shape[2], go.shape[3]
    mid = parts // 2
    n_dev = gi.shape[1]
    head = kc_ref.shape[1]
    q_width = wq.shape[0] - 2 * head
    ff = wo.shape[0] - q_width
    chunk = wg0.shape[0]

    dp, tp = lax.axis_index("dp"), lax.axis_index("tp")
    core, x, y = lax.rem(dp, 2), dp // 2, tp
    a = (1 - core) * x + core * y
    b = (1 - core) * y + core * x

    def place(za, zb, c):
        zx = (1 - c) * za + c * zb
        zy = (1 - c) * zb + c * za
        return zx * 2 + c, zy

    def device(za, zb):
        zdp, ztp = place(lax.rem(za + n, n), lax.rem(zb + n, n), core)
        return {"dp": zdp, "tp": ztp}

    def shard(za, zb, c):
        zdp, ztp = place(za, zb, c)
        return zdp * n + ztp

    partner = {"dp": x * 2 + 1 - core, "tp": tp}
    bufs = (gi, go)
    me = dp * n + tp

    own = []
    for p in range(parts):
        own.append(pltpu.make_async_copy(wi_hbm.at[:, pl.ds(p * lanes, lanes)], gi.at[p, me], own_sem.at[p]))
    for h in range(2):
        own.append(pltpu.make_async_copy(wo_hbm.at[:, pl.ds(h * half, half)], go.at[h, me], own_sem.at[parts + h]))
    for copy in own:
        copy.start()
    x_in = [pltpu.make_async_copy(x_hbm.at[r], x_v.at[r], x_sem.at[r]) for r in range(n_req)]
    for copy in x_in:
        copy.start()

    barrier = pltpu.get_barrier_semaphore()
    for dev in (device(a + 1, b), device(a - 1, b), device(a, b + 1), device(a, b - 1), partner):
        pl.semaphore_signal(barrier, inc=1, device_id=dev, device_id_type=MESH)
    pl.semaphore_wait(barrier, 5)
    for copy in own:
        copy.wait()

    def piece(rnd, h, idx):
        return gi.at[pl.ds(h * mid, mid), idx] if rnd == 0 else go.at[h, idx]

    def first_ring(rnd):
        return Ring(n, a, device(a + 1, b), device(a - 1, b),
                    lambda z, h: piece(rnd, h, shard(z, b, core)),
                    lambda k: send_sem.at[rnd, 0, k], lambda k: recv_sem.at[rnd, 0, k])

    def second_ring(rnd, s):
        return Ring(n, b, device(a, b + 1), device(a, b - 1),
                    lambda z, h: piece(rnd, h, shard(s, z, core)),
                    lambda k: send_sem.at[rnd, 1 + s, k], lambda k: recv_sem.at[rnd, 1 + s, k])

    def pair_copy(rnd, s, k, mine):
        if mine:
            idx = shard(s, lax.rem(b + k, n), core)
        else:
            idx = shard(s, lax.rem(a + k, n), 1 - core)
        ref = bufs[rnd].at[:, idx]
        return pltpu.make_async_remote_copy(
            src_ref=ref, dst_ref=ref, send_sem=psend_sem.at[rnd, s, k], recv_sem=precv_sem.at[rnd, s, k],
            device_id=partner, device_id_type=MESH)

    last = first_ring(1)

    def finish_second(rnd, s):
        second_ring(rnd, s).finish()
        for k in range(1, n):
            pair_copy(rnd, s, k, True).start()

    def start_second(rnd, s):
        second_ring(rnd, s).start()
        pair_copy(rnd, s, 0, True).start()

    def from_partner(rnd, s):
        for k in range(n):
            pair_copy(rnd, s, k, False).wait_recv()

    RIGHT, LEFT = 0, 1
    to_right, to_left = range(mid), range(mid, parts)

    def piece_copy(stage, way, p, back, arriving=False):
        step = back + (1 if arriving else 0)
        pos = b if stage else a
        z = lax.rem(pos + n - step, n) if way == RIGHT else lax.rem(pos + step, n)
        ref = gi.at[p, shard(0, z, core) if stage else shard(z, b, core)]
        sem = p if back == 0 else parts + (p if way == RIGHT else p - mid)
        sign = 1 if way == RIGHT else -1
        return pltpu.make_async_remote_copy(
            src_ref=ref, dst_ref=ref, send_sem=qsend_sem.at[stage, way, sem], recv_sem=qrecv_sem.at[stage, way, sem],
            device_id=device(a, b + sign) if stage else device(a + sign, b), device_id_type=MESH)

    def send(stage, way, p, back=0):
        piece_copy(stage, way, p, back).start()

    def arrive(stage, way, p, back=0):
        piece_copy(stage, way, p, back, True).wait_recv()

    def own_all(way):
        for p in (*to_right, *to_left) if way == RIGHT else (*to_left, *to_right):
            send(0, way, p)

    def forward_all(way):
        for p in to_right if way == RIGHT else to_left:
            arrive(0, way, p)
            send(0, way, p, 1)

    def pass_on(way, p):
        arrive(1, way, p)
        send(1, way, p, 1)

    def first_step(role, i):
        mixed_order = tuple(p for pair in zip(to_right, to_left) for p in pair)
        order = {1: (*to_right, *to_left), n - 1: (*to_left, *to_right)}.get(role, mixed_order)
        p = order[i]
        if role == 1:
            arrive(0, RIGHT, p)
            if p in to_right:
                send(0, RIGHT, p, 1)
        elif role == n - 1:
            arrive(0, LEFT, p)
            if p in to_left:
                send(0, LEFT, p, 1)
        elif role:
            arrive(0, RIGHT if p in to_right else LEFT, p, 1)
        send(1, RIGHT, p)
        send(1, LEFT, p)
        if role == 1 and i == mid - 1:
            own_all(RIGHT)
        if role == n - 1 and i == mid - 1:
            own_all(LEFT)
        if i >= mid:
            if role == 1:
                pass_on(RIGHT, i - mid)
            elif role == n - 1:
                pass_on(LEFT, i)
            elif i == mid:
                pass_on(RIGHT, 0)
                pass_on(LEFT, mid)
            elif i == parts - 1:
                for j in range(1, mid):
                    pass_on(RIGHT, j)
                    pass_on(LEFT, mid + j)

    def on_role(role, fn):
        pl.when(a == role)(fn)

    on_role(0, lambda: (own_all(RIGHT), own_all(LEFT)) and None)
    on_role(1, lambda: own_all(LEFT))
    on_role(n - 1, lambda: own_all(RIGHT))
    on_role(2, lambda: (own_all(RIGHT), own_all(LEFT)) and None)

    gain = gain_ref[...].reshape(1, d)
    ln_rows = 128
    per_req = seq // ln_rows

    def norm_rows(first, count):
        def body(i, carry):
            j = first + i
            r = j // per_req
            rows = pl.ds(pl.multiple_of((j - r * per_req) * ln_rows, ln_rows), ln_rows)
            xw = x_v[r, rows, :].astype(F32)
            cen = xw - jnp.mean(xw, axis=-1, keepdims=True)
            var = jnp.mean(cen * cen, axis=-1, keepdims=True)
            h_v[r, rows, :] = (cen * lax.rsqrt(var + LN_EPS) * gain).astype(BF16)
            return carry
        lax.fori_loop(0, count, body, 0)

    for copy in x_in:
        copy.wait()
    blocks = n_req * per_req
    share = blocks // (parts + 2)
    norm_rows(0, blocks - share * parts)
    for i in range(parts):
        for role in range(n):
            on_role(role, functools.partial(first_step, role, i))
        norm_rows(blocks - share * (parts - i), share)
    pair_copy(0, 0, 0, True).start()
    on_role(1, lambda: [pass_on(LEFT, p) for p in to_left] and None)
    on_role(n - 1, lambda: [pass_on(RIGHT, p) for p in to_right] and None)

    pl.when(a != 1)(lambda: forward_all(RIGHT))
    pl.when(a != n - 1)(lambda: forward_all(LEFT))

    @pl.when(a != 1)
    def _():
        for p in to_left:
            arrive(0, RIGHT, p)

    @pl.when(a != n - 1)
    def _():
        for p in to_right:
            arrive(0, LEFT, p)

    step_a = 1 + a // (n - 1)
    step_b = 3 - step_a
    start_second(0, step_a)

    for p in to_left:
        arrive(1, RIGHT, p)
    pair_copy(0, 0, n - 1, True).start()
    for p in to_right:
        arrive(1, LEFT, p)
    pair_copy(0, 0, 1, True).start()
    for p in to_right:
        arrive(1, RIGHT, p, 1)
    for p in to_left:
        arrive(1, LEFT, p, 1)
    pair_copy(0, 0, 2, True).start()

    def forward_second(rnd, s):
        second_ring(rnd, s).forward()

    @pl.when(a != 2)
    def _():
        for p in to_right:
            arrive(0, RIGHT, p, 1)
        for p in to_left:
            arrive(0, LEFT, p, 1)
    forward_second(0, step_a)
    start_second(0, step_b)
    from_partner(0, 0)

    def assemble(dst, src, rows_per, start, count):
        row = start
        while row < start + count:
            blk, r0 = row // rows_per, row % rows_per
            take = min(rows_per - r0, start + count - row)
            width = src.shape[3]
            for h in range(src.shape[0]):
                dst[row - start:row - start + take, h * width:(h + 1) * width] = src[h, blk, r0:r0 + take, :]
            row += take

    assemble(wq, gi, in_rows, 0, q_width + 2 * head)

    hd2 = head // 2
    scale = float(head ** -0.5 * np.log2(np.e))
    blk = 128
    n_blk = seq // blk
    key_idx = lax.broadcasted_iota(jnp.int32, (blk, blk), 0)
    qry_idx = lax.broadcasted_iota(jnp.int32, (blk, blk), 1)

    def rotate(u):
        cos, sin = cos_ref[...], sin_ref[...]
        first, second = u[:hd2].astype(F32), u[hd2:].astype(F32)
        return jnp.concatenate([first * cos - second * sin, second * cos + first * sin], axis=0).astype(BF16)

    def scores(row, dst):
        q_rot = rotate(qkv[pl.ds(row, head), :])
        for t in range(0, seq, 2 * blk):
            stop = t + 2 * blk
            dst[:stop, t:stop] = jnp.dot(kt[:stop], q_rot[:, t:stop], preferred_element_type=F32)

    def softmax_pv(src, r):
        outs = []
        for t in range(0, n_blk, 2):
            cols, inv = [], []
            for b_q in (t, t + 1):
                lanes = slice(b_q * blk, (b_q + 1) * blk)
                diag = jnp.where(key_idx <= qry_idx, src[lanes, lanes], -1e30)
                top = jnp.max(diag, axis=0, keepdims=True)
                if b_q:
                    top = jnp.maximum(top, jnp.max(src[:b_q * blk, lanes], axis=0, keepdims=True))
                p_diag = jnp.exp2((diag - top) * scale)
                total = jnp.sum(p_diag, axis=0, keepdims=True)
                parts = [p_diag.astype(BF16)]
                if b_q:
                    p_full = jnp.exp2((src[:b_q * blk, lanes] - top) * scale)
                    total = total + jnp.sum(p_full, axis=0, keepdims=True)
                    parts.insert(0, p_full.astype(BF16))
                if b_q == t:
                    parts.append(jnp.zeros((blk, blk), BF16))
                cols.append(parts[0] if len(parts) == 1 else jnp.concatenate(parts, axis=0))
                inv.append(1.0 / total)
            probs = jnp.concatenate(cols, axis=1)
            out = jnp.dot(vc_ref[r, :, :probs.shape[0]], probs, preferred_element_type=F32)
            outs.append(out * jnp.concatenate(inv, axis=1))
        return jnp.concatenate(outs, axis=1)

    def attend(r, between, after):
        qkv[...] = nt_dot(wq[...], h_v[r]).astype(BF16)
        k_rot = rotate(qkv[q_width:q_width + head, :])
        kc_ref[r] = k_rot
        vc_ref[r] = qkv[q_width + head:, :]
        kt[...] = k_rot.astype(F32).T.astype(BF16)
        scores(0, s_a)

        def body(i, carry):
            row = pl.multiple_of(i * 2 * head, 2 * head)
            scores(row + head, s_b)
            out_a = softmax_pv(s_a, r)
            scores(jnp.minimum(row + 2 * head, q_width - head), s_a)
            out_b = softmax_pv(s_b, r)
            mixed[r, :, pl.ds(row, 2 * head)] = jnp.concatenate([out_a, out_b], axis=0).T.astype(BF16)
            return carry

        pairs = q_width // (2 * head)
        lax.fori_loop(0, pairs // 2, body, 0)
        between()
        lax.fori_loop(pairs // 2, pairs, body, 0)
        after()

    def attend_0_mid():
        forward_second(0, step_b)
        start_second(0, 3)

    def attend_1_mid():
        finish_second(0, step_b)
        forward_second(0, 3)

    mids = (attend_0_mid, attend_1_mid, lambda: finish_second(0, 3), None)
    ends = (lambda: finish_second(0, step_a), last.start, last.forward, None)

    def steps(r, todo):
        for at, fn in enumerate(todo):
            if fn is not None:
                pl.when(r == at)(fn)

    def request(r, carry):
        attend(r, lambda: steps(r, mids), lambda: steps(r, ends))
        return carry

    lax.fori_loop(0, n_req, request, 0)
    last.finish()
    for s in range(n):
        start_second(1, s)
    for s in range(1, n):
        from_partner(0, s)

    gate_at = q_width + 2 * head
    tok = 512
    tiles = seq // tok

    tokens = n_req * seq
    columns = ((wg0, wu0), (wg1, wu1))
    n_chunks = ff // chunk

    def gather_chunk(c):
        wg, wu = columns[c % 2]
        assemble(wg, gi, in_rows, gate_at + c * chunk, chunk)
        assemble(wu, gi, in_rows, gate_at + ff + c * chunk, chunk)

    def mlp_chunk(c):
        wg, wu = columns[c % 2]
        h_t = h_v[...].reshape(tokens, d)
        g = nt_dot(h_t, wg[...]).astype(BF16).astype(F32)
        u = nt_dot(h_t, wu[...]).astype(BF16).astype(F32)
        act = 0.5 * g * (1.0 + jnp.tanh(0.5 * g))
        mixed[:, :, q_width + c * chunk:q_width + (c + 1) * chunk] = (act * u).astype(BF16).reshape(n_req, seq, chunk)

    gather_chunk(0)
    for c in range(n_chunks):
        if c + 1 < n_chunks and c:
            gather_chunk(c + 1)
        mlp_chunk(c)
        if c == 0:
            gather_chunk(1)
        if c == 4:
            forward_second(1, 0)
            forward_second(1, 1)
        if c == 5:
            forward_second(1, 2)
            forward_second(1, 3)
            finish_second(1, 0)
            finish_second(1, 1)
        if c == 7:
            finish_second(1, 2)
            finish_second(1, 3)
    for s in range(n):
        from_partner(1, s)

    assemble(wo, go, out_rows, 0, q_width + ff)

    def y_copy(r, t):
        rows = pl.ds(pl.multiple_of(t * tok, tok), tok)
        return pltpu.make_async_copy(x_v.at[r, rows], y_hbm.at[r, rows], y_sem.at[r, t])

    def out_body(i, carry):
        r = i // tiles
        t = i - r * tiles
        rows = pl.ds(pl.multiple_of(t * tok, tok), tok)
        acc = jnp.dot(mixed[r, rows, :], wo[...], preferred_element_type=F32)
        x_v[r, rows, :] = (x_v[r, rows, :].astype(F32) + acc).astype(BF16)
        y_copy(r, t).start()
        return carry
    lax.fori_loop(0, n_req * tiles, out_body, 0)

    for r in range(n_req):
        for t in range(tiles):
            y_copy(r, t).wait()
    for stage in range(2):
        for way in (RIGHT, LEFT):
            for p in range(parts):
                piece_copy(stage, way, p, 0).wait_send()
            for p in to_right if way == RIGHT else to_left:
                piece_copy(stage, way, p, 1).wait_send()
    last.drain()
    for rnd in range(2):
        for s in range(n):
            if rnd or s:
                second_ring(rnd, s).drain()
            for k in range(n):
                pair_copy(rnd, s, k, True).wait_send()


def rope_tables(seq, head):
    inv_freq = (np.float32(ROPE_BASE) ** (-np.arange(head // 2, dtype=np.float32) * np.float32(2.0) / np.float32(head)))
    angles = inv_freq.astype(np.float32)[:, None] * np.arange(seq, dtype=np.float32)[None, :]
    return np.cos(angles).astype(np.float32), np.sin(angles).astype(np.float32)


def solution(mesh):
    tok_spec = P(('part', 'dp', 'tp'))
    n = mesh.shape['tp']
    n_dev = n * mesh.shape['dp']

    def per_device(x_blk, ln_gain, w_in_blk, w_out_blk):
        n_req, seq, d = x_blk.shape
        in_rows, out_rows = w_in_blk.shape[1], w_out_blk.shape[0]
        ff = 4 * d
        q_width = out_rows * n_dev - ff
        head = (in_rows * n_dev - q_width - 2 * ff) // 2
        chunk = 256
        parts = d // 128
        cos, sin = rope_tables(seq, head)
        vmem = pl.BlockSpec(memory_space=pltpu.VMEM)
        anyw = pl.BlockSpec(memory_space=pl.ANY)
        tiles = seq // 512
        y, kc, vc = pl.pallas_call(
            functools.partial(layer_kernel, n),
            out_shape=(jax.ShapeDtypeStruct(x_blk.shape, BF16),
                       jax.ShapeDtypeStruct((n_req, head, seq), BF16),
                       jax.ShapeDtypeStruct((n_req, head, seq), BF16)),
            in_specs=[anyw, vmem, anyw, anyw, vmem, vmem],
            out_specs=(anyw, vmem, vmem),
            scratch_shapes=[
                pltpu.VMEM((n_req, seq, d), BF16),
                pltpu.VMEM((n_req, seq, d), BF16),
                pltpu.VMEM((n_req, seq, q_width + ff), BF16),
                pltpu.VMEM((parts, n_dev, in_rows, d // parts), BF16),
                pltpu.VMEM((2, n_dev, out_rows, d // 2), BF16),
                pltpu.VMEM((q_width + 2 * head, d), BF16),
                pltpu.VMEM((chunk, d), BF16),
                pltpu.VMEM((chunk, d), BF16),
                pltpu.VMEM((chunk, d), BF16),
                pltpu.VMEM((chunk, d), BF16),
                pltpu.VMEM((q_width + ff, d), BF16),
                pltpu.VMEM((q_width + 2 * head, seq), BF16),
                pltpu.VMEM((seq, head), BF16),
                pltpu.VMEM((seq, seq), F32),
                pltpu.VMEM((seq, seq), F32),
                pltpu.SemaphoreType.DMA((n_req,)),
                pltpu.SemaphoreType.DMA((parts + 2,)),
                pltpu.SemaphoreType.DMA((n_req, tiles)),
                pltpu.SemaphoreType.DMA((2, 1 + n, 6)),
                pltpu.SemaphoreType.DMA((2, 1 + n, 6)),
                pltpu.SemaphoreType.DMA((2, n, n)),
                pltpu.SemaphoreType.DMA((2, n, n)),
                pltpu.SemaphoreType.DMA((2, 2, parts + parts // 2)),
                pltpu.SemaphoreType.DMA((2, 2, parts + parts // 2)),
            ],
            compiler_params=pltpu.CompilerParams(
                collective_id=0, has_side_effects=True,
                vmem_limit_bytes=63 * 1024 * 1024),
        )(x_blk, ln_gain, w_in_blk.T, w_out_blk, cos, sin)
        return y, kc.swapaxes(1, 2), vc.swapaxes(1, 2)

    return jax.shard_map(per_device, mesh=mesh,
                         in_specs=(tok_spec, P(), P(None, ('dp', 'tp')), P(('dp', 'tp'), None)),
                         out_specs=(tok_spec, tok_spec, tok_spec), check_vma=False)
```

```python
import functools

import jax
import jax.numpy as jnp
import numpy as np
from jax import lax
from jax.experimental import pallas as pl
from jax.experimental.pallas import tpu as pltpu
from jax.sharding import PartitionSpec as P

LN_EPS = 1e-6
ROPE_BASE = 10000.0
MESH = pl.DeviceIdType.MESH
F32 = jnp.float32
BF16 = jnp.bfloat16


def nt_dot(lhs, rhs):
    return lax.dot_general(lhs, rhs, (((1,), (1,)), ((), ())), preferred_element_type=F32)


class Ring:
    def __init__(self, n, pos, right, left, block, send, recv):
        self.n, self.pos, self.right, self.left = n, pos, right, left
        self.block, self.send, self.recv = block, send, recv
        self.routes = ((0, 0, True), (0, 1, True), (1, 0, True), (0, 1, False), (0, 0, False), (1, 1, False))

    def _copy(self, k, hops):
        back, half, to_right = self.routes[k]
        step = (back + hops) if to_right else self.n - (back + hops)
        z = lax.rem(self.pos - step + 2 * self.n, self.n)
        ref = self.block(z, half)
        return pltpu.make_async_remote_copy(
            src_ref=ref, dst_ref=ref, send_sem=self.send(k), recv_sem=self.recv(k),
            device_id=self.right if to_right else self.left, device_id_type=MESH)

    def start(self):
        for k in (0, 3, 1, 4):
            self._copy(k, 0).start()

    def forward(self):
        self._copy(0, 1).wait_recv()
        self._copy(2, 0).start()
        self._copy(3, 1).wait_recv()
        self._copy(5, 0).start()

    def finish(self):
        for k in (1, 4, 2, 5):
            self._copy(k, 1).wait_recv()

    def drain(self):
        for k in range(6):
            self._copy(k, 0).wait_send()


def layer_kernel(n, x_hbm, gain_ref, wi_hbm, wo_hbm, cos_ref, sin_ref, y_hbm, kc_ref, vc_ref,
                 x_v, h_v, mixed, gi, go, wq, wg0, wu0, wg1, wu1, wo, qkv, kt, s_a, s_b,
                 x_sem, own_sem, y_sem, send_sem, recv_sem, psend_sem, precv_sem, qsend_sem, qrecv_sem):
    n_req, seq, d = x_v.shape
    parts, _, in_rows, lanes = gi.shape
    out_rows, half = go.shape[2], go.shape[3]
    mid = parts // 2
    n_dev = gi.shape[1]
    head = kc_ref.shape[1]
    q_width = wq.shape[0] - 2 * head
    ff = wo.shape[0] - q_width
    chunk = wg0.shape[0]

    dp, tp = lax.axis_index("dp"), lax.axis_index("tp")
    core, x, y = lax.rem(dp, 2), dp // 2, tp
    a = (1 - core) * x + core * y
    b = (1 - core) * y + core * x

    def place(za, zb, c):
        zx = (1 - c) * za + c * zb
        zy = (1 - c) * zb + c * za
        return zx * 2 + c, zy

    def device(za, zb):
        zdp, ztp = place(lax.rem(za + n, n), lax.rem(zb + n, n), core)
        return {"dp": zdp, "tp": ztp}

    def shard(za, zb, c):
        zdp, ztp = place(za, zb, c)
        return zdp * n + ztp

    partner = {"dp": x * 2 + 1 - core, "tp": tp}
    bufs = (gi, go)
    me = dp * n + tp

    own = []
    for p in range(parts):
        own.append(pltpu.make_async_copy(wi_hbm.at[:, pl.ds(p * lanes, lanes)], gi.at[p, me], own_sem.at[p]))
    for h in range(2):
        own.append(pltpu.make_async_copy(wo_hbm.at[:, pl.ds(h * half, half)], go.at[h, me], own_sem.at[parts + h]))
    for copy in own:
        copy.start()
    x_in = [pltpu.make_async_copy(x_hbm.at[r], x_v.at[r], x_sem.at[r]) for r in range(n_req)]
    for copy in x_in:
        copy.start()

    barrier = pltpu.get_barrier_semaphore()
    for dev in (device(a + 1, b), device(a - 1, b), device(a, b + 1), device(a, b - 1), partner):
        pl.semaphore_signal(barrier, inc=1, device_id=dev, device_id_type=MESH)
    pl.semaphore_wait(barrier, 5)
    for copy in own:
        copy.wait()

    def piece(rnd, h, idx):
        return gi.at[pl.ds(h * mid, mid), idx] if rnd == 0 else go.at[h, idx]

    def first_ring(rnd):
        return Ring(n, a, device(a + 1, b), device(a - 1, b),
                    lambda z, h: piece(rnd, h, shard(z, b, core)),
                    lambda k: send_sem.at[rnd, 0, k], lambda k: recv_sem.at[rnd, 0, k])

    def second_ring(rnd, s):
        return Ring(n, b, device(a, b + 1), device(a, b - 1),
                    lambda z, h: piece(rnd, h, shard(s, z, core)),
                    lambda k: send_sem.at[rnd, 1 + s, k], lambda k: recv_sem.at[rnd, 1 + s, k])

    def pair_copy(rnd, s, k, mine):
        if mine:
            idx = shard(s, lax.rem(b + k, n), core)
        else:
            idx = shard(s, lax.rem(a + k, n), 1 - core)
        ref = bufs[rnd].at[:, idx]
        return pltpu.make_async_remote_copy(
            src_ref=ref, dst_ref=ref, send_sem=psend_sem.at[rnd, s, k], recv_sem=precv_sem.at[rnd, s, k],
            device_id=partner, device_id_type=MESH)

    last = first_ring(1)

    def finish_second(rnd, s):
        second_ring(rnd, s).finish()
        for k in range(1, n):
            pair_copy(rnd, s, k, True).start()

    def start_second(rnd, s):
        second_ring(rnd, s).start()
        pair_copy(rnd, s, 0, True).start()

    def from_partner(rnd, s):
        for k in range(n):
            pair_copy(rnd, s, k, False).wait_recv()

    RIGHT, LEFT = 0, 1
    to_right, to_left = range(mid), range(mid, parts)

    def piece_copy(stage, way, p, back, arriving=False):
        step = back + (1 if arriving else 0)
        pos = b if stage else a
        z = lax.rem(pos + n - step, n) if way == RIGHT else lax.rem(pos + step, n)
        ref = gi.at[p, shard(0, z, core) if stage else shard(z, b, core)]
        sem = p if back == 0 else parts + (p if way == RIGHT else p - mid)
        sign = 1 if way == RIGHT else -1
        return pltpu.make_async_remote_copy(
            src_ref=ref, dst_ref=ref, send_sem=qsend_sem.at[stage, way, sem], recv_sem=qrecv_sem.at[stage, way, sem],
            device_id=device(a, b + sign) if stage else device(a + sign, b), device_id_type=MESH)

    def send(stage, way, p, back=0):
        piece_copy(stage, way, p, back).start()

    def arrive(stage, way, p, back=0):
        piece_copy(stage, way, p, back, True).wait_recv()

    def own_all(way):
        for p in (*to_right, *to_left) if way == RIGHT else (*to_left, *to_right):
            send(0, way, p)

    def forward_all(way):
        for p in to_right if way == RIGHT else to_left:
            arrive(0, way, p)
            send(0, way, p, 1)

    def pass_on(way, p):
        arrive(1, way, p)
        send(1, way, p, 1)

    def first_step(role, i):
        mixed_order = tuple(p for pair in zip(to_right, to_left) for p in pair)
        order = {1: (*to_right, *to_left), n - 1: (*to_left, *to_right)}.get(role, mixed_order)
        p = order[i]
        if role == 1:
            arrive(0, RIGHT, p)
            if p in to_right:
                send(0, RIGHT, p, 1)
        elif role == n - 1:
            arrive(0, LEFT, p)
            if p in to_left:
                send(0, LEFT, p, 1)
        elif role:
            arrive(0, RIGHT if p in to_right else LEFT, p, 1)
        send(1, RIGHT, p)
        send(1, LEFT, p)
        if role == 1 and i == mid - 1:
            own_all(RIGHT)
        if role == n - 1 and i == mid - 1:
            own_all(LEFT)
        if i >= mid:
            if role == 1:
                pass_on(RIGHT, i - mid)
            elif role == n - 1:
                pass_on(LEFT, i)
            elif i == mid:
                pass_on(RIGHT, 0)
                pass_on(LEFT, mid)
            elif i == parts - 1:
                for j in range(1, mid):
                    pass_on(RIGHT, j)
                    pass_on(LEFT, mid + j)

    def on_role(role, fn):
        pl.when(a == role)(fn)

    on_role(0, lambda: (own_all(RIGHT), own_all(LEFT)) and None)
    on_role(1, lambda: own_all(LEFT))
    on_role(n - 1, lambda: own_all(RIGHT))
    on_role(2, lambda: (own_all(RIGHT), own_all(LEFT)) and None)

    gain = gain_ref[...].reshape(1, d)
    ln_rows = 128
    per_req = seq // ln_rows

    def norm_rows(first, count):
        def body(i, carry):
            j = first + i
            r = j // per_req
            rows = pl.ds(pl.multiple_of((j - r * per_req) * ln_rows, ln_rows), ln_rows)
            xw = x_v[r, rows, :].astype(F32)
            cen = xw - jnp.mean(xw, axis=-1, keepdims=True)
            var = jnp.mean(cen * cen, axis=-1, keepdims=True)
            h_v[r, rows, :] = (cen * lax.rsqrt(var + LN_EPS) * gain).astype(BF16)
            return carry
        lax.fori_loop(0, count, body, 0)

    for copy in x_in:
        copy.wait()
    blocks = n_req * per_req
    share = blocks // (parts + 2)
    norm_rows(0, blocks - share * parts)
    for i in range(parts):
        for role in range(n):
            on_role(role, functools.partial(first_step, role, i))
        norm_rows(blocks - share * (parts - i), share)
    pair_copy(0, 0, 0, True).start()
    on_role(1, lambda: [pass_on(LEFT, p) for p in to_left] and None)
    on_role(n - 1, lambda: [pass_on(RIGHT, p) for p in to_right] and None)
    pl.when(a != 1)(lambda: forward_all(RIGHT))
    pl.when(a != n - 1)(lambda: forward_all(LEFT))

    @pl.when(a != 1)
    def _():
        for p in to_left:
            arrive(0, RIGHT, p)

    @pl.when(a != n - 1)
    def _():
        for p in to_right:
            arrive(0, LEFT, p)

    step_a = 1 + a // (n - 1)
    step_b = 3 - step_a
    start_second(0, step_a)

    for p in to_left:
        arrive(1, RIGHT, p)
    pair_copy(0, 0, n - 1, True).start()
    for p in to_right:
        arrive(1, LEFT, p)
    pair_copy(0, 0, 1, True).start()
    for p in to_right:
        arrive(1, RIGHT, p, 1)
    for p in to_left:
        arrive(1, LEFT, p, 1)
    pair_copy(0, 0, 2, True).start()

    def far_arrivals():
        for p in to_right:
            arrive(0, RIGHT, p, 1)
        for p in to_left:
            arrive(0, LEFT, p, 1)

    def forward_second(rnd, s):
        second_ring(rnd, s).forward()

    from_partner(0, 0)

    def assemble(dst, src, rows_per, start, count):
        row = start
        while row < start + count:
            blk, r0 = row // rows_per, row % rows_per
            take = min(rows_per - r0, start + count - row)
            width = src.shape[3]
            for h in range(src.shape[0]):
                dst[row - start:row - start + take, h * width:(h + 1) * width] = src[h, blk, r0:r0 + take, :]
            row += take

    assemble(wq, gi, in_rows, 0, q_width + 2 * head)

    hd2 = head // 2
    scale = float(head ** -0.5 * np.log2(np.e))
    blk = 128
    n_blk = seq // blk
    key_idx = lax.broadcasted_iota(jnp.int32, (blk, blk), 0)
    qry_idx = lax.broadcasted_iota(jnp.int32, (blk, blk), 1)

    def rotate(u):
        cos, sin = cos_ref[...], sin_ref[...]
        first, second = u[:hd2].astype(F32), u[hd2:].astype(F32)
        return jnp.concatenate([first * cos - second * sin, second * cos + first * sin], axis=0).astype(BF16)

    def scores(row, dst):
        q_rot = rotate(qkv[pl.ds(row, head), :])
        for t in range(0, seq, 2 * blk):
            stop = t + 2 * blk
            dst[:stop, t:stop] = jnp.dot(kt[:stop], q_rot[:, t:stop], preferred_element_type=F32)

    def softmax_pv(src, r):
        outs = []
        for t in range(0, n_blk, 2):
            cols, inv = [], []
            for b_q in (t, t + 1):
                lanes = slice(b_q * blk, (b_q + 1) * blk)
                diag = jnp.where(key_idx <= qry_idx, src[lanes, lanes], -1e30)
                top = jnp.max(diag, axis=0, keepdims=True)
                if b_q:
                    top = jnp.maximum(top, jnp.max(src[:b_q * blk, lanes], axis=0, keepdims=True))
                p_diag = jnp.exp2((diag - top) * scale)
                total = jnp.sum(p_diag, axis=0, keepdims=True)
                parts = [p_diag.astype(BF16)]
                if b_q:
                    p_full = jnp.exp2((src[:b_q * blk, lanes] - top) * scale)
                    total = total + jnp.sum(p_full, axis=0, keepdims=True)
                    parts.insert(0, p_full.astype(BF16))
                if b_q == t:
                    parts.append(jnp.zeros((blk, blk), BF16))
                cols.append(parts[0] if len(parts) == 1 else jnp.concatenate(parts, axis=0))
                inv.append(1.0 / total)
            probs = jnp.concatenate(cols, axis=1)
            out = jnp.dot(vc_ref[r, :, :probs.shape[0]], probs, preferred_element_type=F32)
            outs.append(out * jnp.concatenate(inv, axis=1))
        return jnp.concatenate(outs, axis=1)

    def attend(r, between, after):
        qkv[...] = nt_dot(wq[...], h_v[r]).astype(BF16)
        k_rot = rotate(qkv[q_width:q_width + head, :])
        kc_ref[r] = k_rot
        vc_ref[r] = qkv[q_width + head:, :]
        kt[...] = k_rot.astype(F32).T.astype(BF16)
        scores(0, s_a)

        def body(i, carry):
            row = pl.multiple_of(i * 2 * head, 2 * head)
            scores(row + head, s_b)
            out_a = softmax_pv(s_a, r)
            scores(jnp.minimum(row + 2 * head, q_width - head), s_a)
            out_b = softmax_pv(s_b, r)
            mixed[r, :, pl.ds(row, 2 * head)] = jnp.concatenate([out_a, out_b], axis=0).T.astype(BF16)
            return carry

        pairs = q_width // (2 * head)
        lax.fori_loop(0, pairs // 2, body, 0)
        between()
        lax.fori_loop(pairs // 2, pairs, body, 0)
        after()

    def attend_0_mid():
        pl.when(a != 2)(far_arrivals)
        start_second(0, step_b)

    def attend_1_mid():
        forward_second(0, step_b)
        start_second(0, 3)

    def attend_2_end():
        finish_second(0, step_b)
        forward_second(0, 3)

    mids = (attend_0_mid, attend_1_mid, lambda: finish_second(0, step_a), last.start)
    ends = (lambda: forward_second(0, step_a), None, attend_2_end, lambda: finish_second(0, 3))

    def steps(r, todo):
        for at, fn in enumerate(todo):
            if fn is not None:
                pl.when(r == at)(fn)

    def request(r, carry):
        attend(r, lambda: steps(r, mids), lambda: steps(r, ends))
        return carry

    lax.fori_loop(0, n_req, request, 0)
    last.forward()
    from_partner(0, 1)
    from_partner(0, 2)

    gate_at = q_width + 2 * head
    tok = 512
    tiles = seq // tok

    tokens = n_req * seq
    columns = ((wg0, wu0), (wg1, wu1))
    n_chunks = ff // chunk

    def gather_chunk(c):
        wg, wu = columns[c % 2]
        assemble(wg, gi, in_rows, gate_at + c * chunk, chunk)
        assemble(wu, gi, in_rows, gate_at + ff + c * chunk, chunk)

    def mlp_chunk(c):
        wg, wu = columns[c % 2]
        h_t = h_v[...].reshape(tokens, d)
        g = nt_dot(h_t, wg[...]).astype(BF16).astype(F32)
        u = nt_dot(h_t, wu[...]).astype(BF16).astype(F32)
        act = 0.5 * g * (1.0 + jnp.tanh(0.5 * g))
        mixed[:, :, q_width + c * chunk:q_width + (c + 1) * chunk] = (act * u).astype(BF16).reshape(n_req, seq, chunk)

    gather_chunk(0)
    for c in range(n_chunks):
        if c == 1:
            from_partner(0, 3)
        if c + 1 < n_chunks and c:
            gather_chunk(c + 1)
        mlp_chunk(c)
        if c == 0:
            gather_chunk(1)
        if c == 1:
            last.finish()
            for s in range(n):
                start_second(1, s)
        if c == 4:
            forward_second(1, 0)
            forward_second(1, 1)
        if c == 6:
            forward_second(1, 2)
            forward_second(1, 3)
            finish_second(1, 0)
            finish_second(1, 1)
        if c == 8:
            finish_second(1, 2)
            finish_second(1, 3)
    for s in range(n):
        from_partner(1, s)

    assemble(wo, go, out_rows, 0, q_width + ff)

    def y_copy(r, t):
        rows = pl.ds(pl.multiple_of(t * tok, tok), tok)
        return pltpu.make_async_copy(x_v.at[r, rows], y_hbm.at[r, rows], y_sem.at[r, t])

    def out_body(i, carry):
        r = i // tiles
        t = i - r * tiles
        rows = pl.ds(pl.multiple_of(t * tok, tok), tok)
        acc = jnp.dot(mixed[r, rows, :], wo[...], preferred_element_type=F32)
        x_v[r, rows, :] = (x_v[r, rows, :].astype(F32) + acc).astype(BF16)
        y_copy(r, t).start()
        return carry
    lax.fori_loop(0, n_req * tiles, out_body, 0)

    for r in range(n_req):
        for t in range(tiles):
            y_copy(r, t).wait()
    for stage in range(2):
        for way in (RIGHT, LEFT):
            for p in range(parts):
                piece_copy(stage, way, p, 0).wait_send()
            for p in to_right if way == RIGHT else to_left:
                piece_copy(stage, way, p, 1).wait_send()
    last.drain()
    for rnd in range(2):
        for s in range(n):
            if rnd or s:
                second_ring(rnd, s).drain()
            for k in range(n):
                pair_copy(rnd, s, k, True).wait_send()


def rope_tables(seq, head):
    inv_freq = (np.float32(ROPE_BASE) ** (-np.arange(head // 2, dtype=np.float32) * np.float32(2.0) / np.float32(head)))
    angles = inv_freq.astype(np.float32)[:, None] * np.arange(seq, dtype=np.float32)[None, :]
    return np.cos(angles).astype(np.float32), np.sin(angles).astype(np.float32)


def solution(mesh):
    tok_spec = P(('part', 'dp', 'tp'))
    n = mesh.shape['tp']
    n_dev = n * mesh.shape['dp']

    def per_device(x_blk, ln_gain, w_in_blk, w_out_blk):
        n_req, seq, d = x_blk.shape
        in_rows, out_rows = w_in_blk.shape[1], w_out_blk.shape[0]
        ff = 4 * d
        q_width = out_rows * n_dev - ff
        head = (in_rows * n_dev - q_width - 2 * ff) // 2
        chunk = 256
        parts = d // 128
        cos, sin = rope_tables(seq, head)
        vmem = pl.BlockSpec(memory_space=pltpu.VMEM)
        anyw = pl.BlockSpec(memory_space=pl.ANY)
        tiles = seq // 512
        y, kc, vc = pl.pallas_call(
            functools.partial(layer_kernel, n),
            out_shape=(jax.ShapeDtypeStruct(x_blk.shape, BF16),
                       jax.ShapeDtypeStruct((n_req, head, seq), BF16),
                       jax.ShapeDtypeStruct((n_req, head, seq), BF16)),
            in_specs=[anyw, vmem, anyw, anyw, vmem, vmem],
            out_specs=(anyw, vmem, vmem),
            scratch_shapes=[
                pltpu.VMEM((n_req, seq, d), BF16),
                pltpu.VMEM((n_req, seq, d), BF16),
                pltpu.VMEM((n_req, seq, q_width + ff), BF16),
                pltpu.VMEM((parts, n_dev, in_rows, d // parts), BF16),
                pltpu.VMEM((2, n_dev, out_rows, d // 2), BF16),
                pltpu.VMEM((q_width + 2 * head, d), BF16),
                pltpu.VMEM((chunk, d), BF16),
                pltpu.VMEM((chunk, d), BF16),
                pltpu.VMEM((chunk, d), BF16),
                pltpu.VMEM((chunk, d), BF16),
                pltpu.VMEM((q_width + ff, d), BF16),
                pltpu.VMEM((q_width + 2 * head, seq), BF16),
                pltpu.VMEM((seq, head), BF16),
                pltpu.VMEM((seq, seq), F32),
                pltpu.VMEM((seq, seq), F32),
                pltpu.SemaphoreType.DMA((n_req,)),
                pltpu.SemaphoreType.DMA((parts + 2,)),
                pltpu.SemaphoreType.DMA((n_req, tiles)),
                pltpu.SemaphoreType.DMA((2, 1 + n, 6)),
                pltpu.SemaphoreType.DMA((2, 1 + n, 6)),
                pltpu.SemaphoreType.DMA((2, n, n)),
                pltpu.SemaphoreType.DMA((2, n, n)),
                pltpu.SemaphoreType.DMA((2, 2, parts + parts // 2)),
                pltpu.SemaphoreType.DMA((2, 2, parts + parts // 2)),
            ],
            compiler_params=pltpu.CompilerParams(
                collective_id=0, has_side_effects=True,
                vmem_limit_bytes=63 * 1024 * 1024),
        )(x_blk, ln_gain, w_in_blk.T, w_out_blk, cos, sin)
        return y, kc.swapaxes(1, 2), vc.swapaxes(1, 2)

    return jax.shard_map(per_device, mesh=mesh,
                         in_specs=(tok_spec, P(), P(None, ('dp', 'tp')), P(('dp', 'tp'), None)),
                         out_specs=(tok_spec, tok_spec, tok_spec), check_vma=False)
```

```python
import functools

import jax
import jax.numpy as jnp
import numpy as np
from jax import lax
from jax.experimental import pallas as pl
from jax.experimental.pallas import tpu as pltpu
from jax.sharding import PartitionSpec as P

LN_EPS = 1e-6
ROPE_BASE = 10000.0
MESH = pl.DeviceIdType.MESH
F32 = jnp.float32
BF16 = jnp.bfloat16


def nt_dot(lhs, rhs):
    return lax.dot_general(lhs, rhs, (((1,), (1,)), ((), ())), preferred_element_type=F32)


class Ring:
    def __init__(self, n, pos, right, left, block, send, recv):
        self.n, self.pos, self.right, self.left = n, pos, right, left
        self.block, self.send, self.recv = block, send, recv
        self.routes = ((0, 0, True), (0, 1, True), (1, 0, True), (0, 1, False), (0, 0, False), (1, 1, False))

    def _copy(self, k, hops):
        back, half, to_right = self.routes[k]
        step = (back + hops) if to_right else self.n - (back + hops)
        z = lax.rem(self.pos - step + 2 * self.n, self.n)
        ref = self.block(z, half)
        return pltpu.make_async_remote_copy(
            src_ref=ref, dst_ref=ref, send_sem=self.send(k), recv_sem=self.recv(k),
            device_id=self.right if to_right else self.left, device_id_type=MESH)

    def start(self):
        for k in (0, 3, 1, 4):
            self._copy(k, 0).start()

    def forward(self):
        self._copy(0, 1).wait_recv()
        self._copy(2, 0).start()
        self._copy(3, 1).wait_recv()
        self._copy(5, 0).start()

    def finish(self):
        for k in (1, 4, 2, 5):
            self._copy(k, 1).wait_recv()

    def drain(self):
        for k in range(6):
            self._copy(k, 0).wait_send()


def layer_kernel(n, x_hbm, gain_ref, wi_hbm, wo_hbm, cos_ref, sin_ref, y_hbm, kc_ref, vc_ref,
                 x_v, h_v, mixed, gi, go, wq, wg0, wu0, wg1, wu1, wo, qkv, kt, s_a, s_b,
                 x_sem, own_sem, y_sem, send_sem, recv_sem, psend_sem, precv_sem, qsend_sem, qrecv_sem):
    n_req, seq, d = x_v.shape
    parts, _, in_rows, lanes = gi.shape
    out_rows, half = go.shape[2], go.shape[3]
    mid = parts // 2
    n_dev = gi.shape[1]
    head = kc_ref.shape[1]
    q_width = wq.shape[0] - 2 * head
    ff = wo.shape[0] - q_width
    chunk = wg0.shape[0]

    dp, tp = lax.axis_index("dp"), lax.axis_index("tp")
    core, x, y = lax.rem(dp, 2), dp // 2, tp
    a = (1 - core) * x + core * y
    b = (1 - core) * y + core * x

    def place(za, zb, c):
        zx = (1 - c) * za + c * zb
        zy = (1 - c) * zb + c * za
        return zx * 2 + c, zy

    def device(za, zb):
        zdp, ztp = place(lax.rem(za + n, n), lax.rem(zb + n, n), core)
        return {"dp": zdp, "tp": ztp}

    def shard(za, zb, c):
        zdp, ztp = place(za, zb, c)
        return zdp * n + ztp

    partner = {"dp": x * 2 + 1 - core, "tp": tp}
    bufs = (gi, go)
    me = dp * n + tp

    own = []
    for p in range(parts):
        own.append(pltpu.make_async_copy(wi_hbm.at[:, pl.ds(p * lanes, lanes)], gi.at[p, me], own_sem.at[p]))
    for h in range(2):
        own.append(pltpu.make_async_copy(wo_hbm.at[:, pl.ds(h * half, half)], go.at[h, me], own_sem.at[parts + h]))
    for copy in own:
        copy.start()
    x_in = [pltpu.make_async_copy(x_hbm.at[r], x_v.at[r], x_sem.at[r]) for r in range(n_req)]
    for copy in x_in:
        copy.start()

    barrier = pltpu.get_barrier_semaphore()
    for dev in (device(a + 1, b), device(a - 1, b), device(a, b + 1), device(a, b - 1), partner):
        pl.semaphore_signal(barrier, inc=1, device_id=dev, device_id_type=MESH)
    pl.semaphore_wait(barrier, 5)
    for copy in own:
        copy.wait()

    def piece(rnd, h, idx):
        return gi.at[pl.ds(h * mid, mid), idx] if rnd == 0 else go.at[h, idx]

    def first_ring(rnd):
        return Ring(n, a, device(a + 1, b), device(a - 1, b),
                    lambda z, h: piece(rnd, h, shard(z, b, core)),
                    lambda k: send_sem.at[rnd, 0, k], lambda k: recv_sem.at[rnd, 0, k])

    def second_ring(rnd, s):
        return Ring(n, b, device(a, b + 1), device(a, b - 1),
                    lambda z, h: piece(rnd, h, shard(s, z, core)),
                    lambda k: send_sem.at[rnd, 1 + s, k], lambda k: recv_sem.at[rnd, 1 + s, k])

    def pair_copy(rnd, s, k, mine):
        if mine:
            idx = shard(s, lax.rem(b + k, n), core)
        else:
            idx = shard(s, lax.rem(a + k, n), 1 - core)
        ref = bufs[rnd].at[:, idx]
        return pltpu.make_async_remote_copy(
            src_ref=ref, dst_ref=ref, send_sem=psend_sem.at[rnd, s, k], recv_sem=precv_sem.at[rnd, s, k],
            device_id=partner, device_id_type=MESH)

    last = first_ring(1)

    def finish_second(rnd, s):
        second_ring(rnd, s).finish()
        for k in range(1, n):
            pair_copy(rnd, s, k, True).start()

    def start_second(rnd, s):
        second_ring(rnd, s).start()
        pair_copy(rnd, s, 0, True).start()

    def from_partner(rnd, s):
        for k in range(n):
            pair_copy(rnd, s, k, False).wait_recv()

    RIGHT, LEFT = 0, 1
    to_right, to_left = range(mid), range(mid, parts)

    def piece_copy(stage, way, p, back, arriving=False):
        step = back + (1 if arriving else 0)
        pos = b if stage else a
        z = lax.rem(pos + n - step, n) if way == RIGHT else lax.rem(pos + step, n)
        ref = gi.at[p, shard(0, z, core) if stage else shard(z, b, core)]
        sem = p if back == 0 else parts + (p if way == RIGHT else p - mid)
        sign = 1 if way == RIGHT else -1
        return pltpu.make_async_remote_copy(
            src_ref=ref, dst_ref=ref, send_sem=qsend_sem.at[stage, way, sem], recv_sem=qrecv_sem.at[stage, way, sem],
            device_id=device(a, b + sign) if stage else device(a + sign, b), device_id_type=MESH)

    def send(stage, way, p, back=0):
        piece_copy(stage, way, p, back).start()

    def arrive(stage, way, p, back=0):
        piece_copy(stage, way, p, back, True).wait_recv()

    def own_all(way):
        for p in (*to_right, *to_left) if way == RIGHT else (*to_left, *to_right):
            send(0, way, p)

    def forward_all(way):
        for p in to_right if way == RIGHT else to_left:
            arrive(0, way, p)
            send(0, way, p, 1)

    def pass_on(way, p):
        arrive(1, way, p)
        send(1, way, p, 1)

    def first_step(role, i):
        mixed_order = tuple(p for pair in zip(to_right, to_left) for p in pair)
        order = {1: (*to_right, *to_left), n - 1: (*to_left, *to_right)}.get(role, mixed_order)
        p = order[i]
        if role == 1:
            arrive(0, RIGHT, p)
            if p in to_right:
                send(0, RIGHT, p, 1)
        elif role == n - 1:
            arrive(0, LEFT, p)
            if p in to_left:
                send(0, LEFT, p, 1)
        elif role:
            arrive(0, RIGHT if p in to_right else LEFT, p, 1)
        send(1, RIGHT, p)
        send(1, LEFT, p)
        if role == 1 and i == mid - 1:
            own_all(RIGHT)
        if role == n - 1 and i == mid - 1:
            own_all(LEFT)
        if i >= mid:
            if role == 1:
                pass_on(RIGHT, i - mid)
            elif role == n - 1:
                pass_on(LEFT, i)
            elif i == mid:
                pass_on(RIGHT, 0)
                pass_on(LEFT, mid)
            elif i == parts - 1:
                for j in range(1, mid):
                    pass_on(RIGHT, j)
                    pass_on(LEFT, mid + j)

    def on_role(role, fn):
        pl.when(a == role)(fn)

    on_role(0, lambda: (own_all(RIGHT), own_all(LEFT)) and None)
    on_role(1, lambda: own_all(LEFT))
    on_role(n - 1, lambda: own_all(RIGHT))
    on_role(2, lambda: (own_all(RIGHT), own_all(LEFT)) and None)

    gain = gain_ref[...].reshape(1, d)
    ln_rows = 128
    per_req = seq // ln_rows

    def norm_rows(first, count):
        def body(i, carry):
            j = first + i
            r = j // per_req
            rows = pl.ds(pl.multiple_of((j - r * per_req) * ln_rows, ln_rows), ln_rows)
            xw = x_v[r, rows, :].astype(F32)
            cen = xw - jnp.mean(xw, axis=-1, keepdims=True)
            var = jnp.mean(cen * cen, axis=-1, keepdims=True)
            h_v[r, rows, :] = (cen * lax.rsqrt(var + LN_EPS) * gain).astype(BF16)
            return carry
        lax.fori_loop(0, count, body, 0)

    for copy in x_in:
        copy.wait()
    blocks = n_req * per_req
    share = blocks // (parts + 2)
    norm_rows(0, blocks - share * parts)
    for i in range(parts):
        for role in range(n):
            on_role(role, functools.partial(first_step, role, i))
        norm_rows(blocks - share * (parts - i), share)
    pair_copy(0, 0, 0, True).start()
    on_role(1, lambda: [pass_on(LEFT, p) for p in to_left] and None)
    on_role(n - 1, lambda: [pass_on(RIGHT, p) for p in to_right] and None)
    pl.when(a != 1)(lambda: forward_all(RIGHT))
    pl.when(a != n - 1)(lambda: forward_all(LEFT))

    @pl.when(a != 1)
    def _():
        for p in to_left:
            arrive(0, RIGHT, p)

    @pl.when(a != n - 1)
    def _():
        for p in to_right:
            arrive(0, LEFT, p)

    step_a = 1 + a // (n - 1)
    step_b = 3 - step_a
    start_second(0, step_a)

    for p in to_left:
        arrive(1, RIGHT, p)
    pair_copy(0, 0, n - 1, True).start()
    for p in to_right:
        arrive(1, LEFT, p)
    pair_copy(0, 0, 1, True).start()
    for p in to_right:
        arrive(1, RIGHT, p, 1)
    for p in to_left:
        arrive(1, LEFT, p, 1)
    pair_copy(0, 0, 2, True).start()

    def far_arrivals():
        for p in to_right:
            arrive(0, RIGHT, p, 1)
        for p in to_left:
            arrive(0, LEFT, p, 1)

    def forward_second(rnd, s):
        second_ring(rnd, s).forward()

    from_partner(0, 0)

    def assemble(dst, src, rows_per, start, count):
        row = start
        while row < start + count:
            blk, r0 = row // rows_per, row % rows_per
            take = min(rows_per - r0, start + count - row)
            width = src.shape[3]
            for h in range(src.shape[0]):
                dst[row - start:row - start + take, h * width:(h + 1) * width] = src[h, blk, r0:r0 + take, :]
            row += take

    assemble(wq, gi, in_rows, 0, q_width + 2 * head)

    hd2 = head // 2
    scale = float(head ** -0.5 * np.log2(np.e))
    blk = 128
    n_blk = seq // blk
    key_idx = lax.broadcasted_iota(jnp.int32, (blk, blk), 0)
    qry_idx = lax.broadcasted_iota(jnp.int32, (blk, blk), 1)

    def rotate(u):
        cos, sin = cos_ref[...], sin_ref[...]
        first, second = u[:hd2].astype(F32), u[hd2:].astype(F32)
        return jnp.concatenate([first * cos - second * sin, second * cos + first * sin], axis=0).astype(BF16)

    def scores(row, dst):
        q_rot = rotate(qkv[pl.ds(row, head), :])
        for t in range(0, seq, 2 * blk):
            stop = t + 2 * blk
            dst[:stop, t:stop] = jnp.dot(kt[:stop], q_rot[:, t:stop], preferred_element_type=F32)

    def softmax_pv(src, r):
        outs = []
        for t in range(0, n_blk, 2):
            cols, inv = [], []
            for b_q in (t, t + 1):
                lanes = slice(b_q * blk, (b_q + 1) * blk)
                diag = jnp.where(key_idx <= qry_idx, src[lanes, lanes], -1e30)
                top = jnp.max(diag, axis=0, keepdims=True)
                if b_q:
                    top = jnp.maximum(top, jnp.max(src[:b_q * blk, lanes], axis=0, keepdims=True))
                p_diag = jnp.exp2((diag - top) * scale)
                total = jnp.sum(p_diag, axis=0, keepdims=True)
                parts = [p_diag.astype(BF16)]
                if b_q:
                    p_full = jnp.exp2((src[:b_q * blk, lanes] - top) * scale)
                    total = total + jnp.sum(p_full, axis=0, keepdims=True)
                    parts.insert(0, p_full.astype(BF16))
                if b_q == t:
                    parts.append(jnp.zeros((blk, blk), BF16))
                cols.append(parts[0] if len(parts) == 1 else jnp.concatenate(parts, axis=0))
                inv.append(1.0 / total)
            probs = jnp.concatenate(cols, axis=1)
            out = jnp.dot(vc_ref[r, :, :probs.shape[0]], probs, preferred_element_type=F32)
            outs.append(out * jnp.concatenate(inv, axis=1))
        return jnp.concatenate(outs, axis=1)

    def attend(r, between, after):
        qkv[...] = nt_dot(wq[...], h_v[r]).astype(BF16)
        k_rot = rotate(qkv[q_width:q_width + head, :])
        kc_ref[r] = k_rot
        vc_ref[r] = qkv[q_width + head:, :]
        kt[...] = k_rot.astype(F32).T.astype(BF16)
        scores(0, s_a)

        def body(i, carry):
            row = pl.multiple_of(i * 2 * head, 2 * head)
            scores(row + head, s_b)
            out_a = softmax_pv(s_a, r)
            scores(jnp.minimum(row + 2 * head, q_width - head), s_a)
            out_b = softmax_pv(s_b, r)
            mixed[r, :, pl.ds(row, 2 * head)] = jnp.concatenate([out_a, out_b], axis=0).T.astype(BF16)
            return carry

        pairs = q_width // (2 * head)
        lax.fori_loop(0, pairs // 2, body, 0)
        between()
        lax.fori_loop(pairs // 2, pairs, body, 0)
        after()

    def attend_0_mid():
        forward_second(0, step_a)
        pl.when(a != 2)(far_arrivals)
        start_second(0, step_b)

    def attend_1_mid():
        forward_second(0, step_b)
        start_second(0, 3)

    def attend_2_end():
        finish_second(0, step_b)
        forward_second(0, 3)

    mids = (attend_0_mid, attend_1_mid, None, last.start)
    ends = (None, lambda: finish_second(0, step_a), attend_2_end, lambda: finish_second(0, 3))

    def steps(r, todo):
        for at, fn in enumerate(todo):
            if fn is not None:
                pl.when(r == at)(fn)

    def request(r, carry):
        attend(r, lambda: steps(r, mids), lambda: steps(r, ends))
        return carry

    lax.fori_loop(0, n_req, request, 0)
    last.forward()
    from_partner(0, 1)
    from_partner(0, 2)

    gate_at = q_width + 2 * head
    tok = 512
    tiles = seq // tok

    tokens = n_req * seq
    columns = ((wg0, wu0), (wg1, wu1))
    n_chunks = ff // chunk

    def gather_chunk(c):
        wg, wu = columns[c % 2]
        assemble(wg, gi, in_rows, gate_at + c * chunk, chunk)
        assemble(wu, gi, in_rows, gate_at + ff + c * chunk, chunk)

    def mlp_chunk(c):
        wg, wu = columns[c % 2]
        h_t = h_v[...].reshape(tokens, d)
        g = nt_dot(h_t, wg[...]).astype(BF16).astype(F32)
        u = nt_dot(h_t, wu[...]).astype(BF16).astype(F32)
        act = 0.5 * g * (1.0 + jnp.tanh(0.5 * g))
        mixed[:, :, q_width + c * chunk:q_width + (c + 1) * chunk] = (act * u).astype(BF16).reshape(n_req, seq, chunk)

    gather_chunk(0)
    for c in range(n_chunks):
        if c == 1:
            from_partner(0, 3)
        if c + 1 < n_chunks and c:
            gather_chunk(c + 1)
        mlp_chunk(c)
        if c == 0:
            gather_chunk(1)
        if c == 1:
            last.finish()
            for s in range(n):
                start_second(1, s)
        if c == 4:
            forward_second(1, 0)
            forward_second(1, 1)
        if c == 6:
            forward_second(1, 2)
            forward_second(1, 3)
            finish_second(1, 0)
            finish_second(1, 1)
        if c == 8:
            finish_second(1, 2)
            finish_second(1, 3)
    for s in range(n):
        from_partner(1, s)

    assemble(wo, go, out_rows, 0, q_width + ff)

    def y_copy(r, t):
        rows = pl.ds(pl.multiple_of(t * tok, tok), tok)
        return pltpu.make_async_copy(x_v.at[r, rows], y_hbm.at[r, rows], y_sem.at[r, t])

    def out_body(i, carry):
        r = i // tiles
        t = i - r * tiles
        rows = pl.ds(pl.multiple_of(t * tok, tok), tok)
        acc = jnp.dot(mixed[r, rows, :], wo[...], preferred_element_type=F32)
        x_v[r, rows, :] = (x_v[r, rows, :].astype(F32) + acc).astype(BF16)
        y_copy(r, t).start()
        return carry
    lax.fori_loop(0, n_req * tiles, out_body, 0)

    for r in range(n_req):
        for t in range(tiles):
            y_copy(r, t).wait()
    for stage in range(2):
        for way in (RIGHT, LEFT):
            for p in range(parts):
                piece_copy(stage, way, p, 0).wait_send()
            for p in to_right if way == RIGHT else to_left:
                piece_copy(stage, way, p, 1).wait_send()
    last.drain()
    for rnd in range(2):
        for s in range(n):
            if rnd or s:
                second_ring(rnd, s).drain()
            for k in range(n):
                pair_copy(rnd, s, k, True).wait_send()


def rope_tables(seq, head):
    inv_freq = (np.float32(ROPE_BASE) ** (-np.arange(head // 2, dtype=np.float32) * np.float32(2.0) / np.float32(head)))
    angles = inv_freq.astype(np.float32)[:, None] * np.arange(seq, dtype=np.float32)[None, :]
    return np.cos(angles).astype(np.float32), np.sin(angles).astype(np.float32)


def solution(mesh):
    tok_spec = P(('part', 'dp', 'tp'))
    n = mesh.shape['tp']
    n_dev = n * mesh.shape['dp']

    def per_device(x_blk, ln_gain, w_in_blk, w_out_blk):
        n_req, seq, d = x_blk.shape
        in_rows, out_rows = w_in_blk.shape[1], w_out_blk.shape[0]
        ff = 4 * d
        q_width = out_rows * n_dev - ff
        head = (in_rows * n_dev - q_width - 2 * ff) // 2
        chunk = 256
        parts = d // 128
        cos, sin = rope_tables(seq, head)
        vmem = pl.BlockSpec(memory_space=pltpu.VMEM)
        anyw = pl.BlockSpec(memory_space=pl.ANY)
        tiles = seq // 512
        y, kc, vc = pl.pallas_call(
            functools.partial(layer_kernel, n),
            out_shape=(jax.ShapeDtypeStruct(x_blk.shape, BF16),
                       jax.ShapeDtypeStruct((n_req, head, seq), BF16),
                       jax.ShapeDtypeStruct((n_req, head, seq), BF16)),
            in_specs=[anyw, vmem, anyw, anyw, vmem, vmem],
            out_specs=(anyw, vmem, vmem),
            scratch_shapes=[
                pltpu.VMEM((n_req, seq, d), BF16),
                pltpu.VMEM((n_req, seq, d), BF16),
                pltpu.VMEM((n_req, seq, q_width + ff), BF16),
                pltpu.VMEM((parts, n_dev, in_rows, d // parts), BF16),
                pltpu.VMEM((2, n_dev, out_rows, d // 2), BF16),
                pltpu.VMEM((q_width + 2 * head, d), BF16),
                pltpu.VMEM((chunk, d), BF16),
                pltpu.VMEM((chunk, d), BF16),
                pltpu.VMEM((chunk, d), BF16),
                pltpu.VMEM((chunk, d), BF16),
                pltpu.VMEM((q_width + ff, d), BF16),
                pltpu.VMEM((q_width + 2 * head, seq), BF16),
                pltpu.VMEM((seq, head), BF16),
                pltpu.VMEM((seq, seq), F32),
                pltpu.VMEM((seq, seq), F32),
                pltpu.SemaphoreType.DMA((n_req,)),
                pltpu.SemaphoreType.DMA((parts + 2,)),
                pltpu.SemaphoreType.DMA((n_req, tiles)),
                pltpu.SemaphoreType.DMA((2, 1 + n, 6)),
                pltpu.SemaphoreType.DMA((2, 1 + n, 6)),
                pltpu.SemaphoreType.DMA((2, n, n)),
                pltpu.SemaphoreType.DMA((2, n, n)),
                pltpu.SemaphoreType.DMA((2, 2, parts + parts // 2)),
                pltpu.SemaphoreType.DMA((2, 2, parts + parts // 2)),
            ],
            compiler_params=pltpu.CompilerParams(
                collective_id=0, has_side_effects=True,
                vmem_limit_bytes=63 * 1024 * 1024),
        )(x_blk, ln_gain, w_in_blk.T, w_out_blk, cos, sin)
        return y, kc.swapaxes(1, 2), vc.swapaxes(1, 2)

    return jax.shard_map(per_device, mesh=mesh,
                         in_specs=(tok_spec, P(), P(None, ('dp', 'tp')), P(('dp', 'tp'), None)),
                         out_specs=(tok_spec, tok_spec, tok_spec), check_vma=False)
```
